128 devices in a mesh: group: 4 (over y), dom: 32 (over x, z, core).
Axes of the slice: x: 4, y: 4, z: 4, core: 2. Of those that a mesh axis runs over, the one named last changes fastest.
Arguments:
- p_start: float32 [4096, 128], P(('group', 'dom')), may hold values from -60 to 60
- r_start: float32 [4096, 128], P(('group', 'dom')), may hold values from -60 to 60
- diag_shift: float32 [4096, 128], P(('group', 'dom')), may hold values from 0.5 to 2
- shifts: float32 [8], replicated, may hold values from 0.5 to 1.5
- block_values: float32 [4096, 6, 128, 128], P(('group', 'dom')), may hold values from -0.21875 to 0.21875
- block_cols: int32 [4096, 6], P(('group', 'dom')), may hold values from 0 to 95, as said below
- live_slots: int32 [4096], P(('group', 'dom')), may hold values from 2 to 6, as said below
- needed: int32 [128, 4, 16], P(('group', 'dom')), may hold values from 0 to 31
Outputs:
- basis: float32 [17, 4096, 128], P(None, ('group', 'dom'))
- gram: float32 [17, 17], replicated
The draws below stay inside these ranges and needn't reach their ends.
Inputs may be any that keep to these rules, and one draw needn't show every extreme that they name: `block_cols`: slot 0 of block row b is the row itself (b mod 32); a value below 32 names a block row of the same device, a value 32 + k * 16 + h names entry h of the device's list k of needed. Devices with dom index 0 never use list 0 in used slots, devices with the last dom index never list 1. Slots from live_slots on hold values in range but are not used. `live_slots`: the first block row of every device uses all 6 slots. needed[d, k] lists the local block rows that device d reads from its source s_k(d), in the order of its extended field.
All inputs are finite; a program needn't handle non-finite values.
Results may differ from the reference program's by a relative error of at most 0.0001.
Values sent between devices are 32-bit elements; how exact they have to be, the bound alone decides.
A program may use at most 64 MiB of HBM per device.

```python
import math
import jax
import jax.numpy as jnp
from jax import lax

BS = 128
S = 8
NB = 6
BR_DEV = 32
HALO = 16
NBLK = 4096
N_GROUP = 4
N_DOM = 32


def rough_vector(key):
    total = BR_DEV * N_GROUP * N_DOM
    owners = (jnp.arange(total) // BR_DEV).astype(jnp.float32)
    rise = jnp.exp(math.log(3.0) * owners / max(N_GROUP * N_DOM - 1, 1))
    cell = jnp.exp(jax.random.uniform(jax.random.fold_in(key, 1), (total, BS), jnp.float32, 0.0, math.log(10.0)))
    base = jax.random.normal(jax.random.fold_in(key, 2), (total, BS), jnp.float32)
    return base * cell * rise[:, None] * 0.25


def draw_p_start(key, part):
    return rough_vector(jax.random.fold_in(key, 101))


def draw_r_start(key, part):
    return rough_vector(jax.random.fold_in(key, 202))


def block_pattern(key):
    base_key = jax.random.fold_in(key, 303)
    total = BR_DEV * N_GROUP * N_DOM
    block_ids = jnp.arange(total, dtype=jnp.int32)
    dom_ids = block_ids // BR_DEV % N_DOM
    live = jax.random.randint(jax.random.fold_in(base_key, 1), (total,), 2, NB + 1)
    live = jnp.where(block_ids % BR_DEV == 0, NB, live).astype(jnp.int32)
    local_pick = jax.random.randint(jax.random.fold_in(base_key, 2), (total, NB), 0, BR_DEV)
    source_pick = jax.random.randint(jax.random.fold_in(base_key, 3), (total, NB), 0, 4)
    entry_pick = jax.random.randint(jax.random.fold_in(base_key, 4), (total, NB), 0, HALO)
    remote_pick = jax.random.randint(jax.random.fold_in(base_key, 5), (total, NB), 0, 2)
    missing = (source_pick == 0) & (dom_ids[:, None] == 0) | (source_pick == 1) & (dom_ids[:, None] == N_DOM - 1)
    remote = (remote_pick == 1) & jnp.logical_not(missing)
    cols = jnp.where(remote, BR_DEV + source_pick * HALO + entry_pick, local_pick)
    cols = cols.at[:, 0].set(block_ids % BR_DEV)
    return (cols.astype(jnp.int32), live)


def draw_block_cols(key, part):
    return block_pattern(key)[0]


def draw_live_slots(key, part):
    return block_pattern(key)[1]


def place_ends(values, stream_key, smallest, largest):
    longest = values.shape.index(max(values.shape))
    spots = []
    for shift in (0, 1):
        where = [jax.random.randint(jax.random.fold_in(stream_key, axis), (), 0, length) for axis, length in enumerate(values.shape)]
        where[longest] = (where[longest] + shift) % values.shape[longest]
        spots.append(tuple(where))
    return values.at[spots[0]].set(smallest).at[spots[1]].set(largest)


def shard_levels(own_key, extent, cuts, smallest, largest):
    def one(dim, parts):
        steps = jax.random.uniform(jax.random.fold_in(jax.random.fold_in(own_key, 6), dim), (parts,), jnp.float32, smallest / len(cuts), largest / len(cuts))
        return jnp.repeat(jnp.exp(steps), extent[dim] // parts).reshape((-1,) + (1,) * (len(extent) - dim - 1))

    level = one(*cuts[0])
    for cut in cuts[1:]:
        level = level * one(*cut)
    return level


def bell_draw(rng, shape, width, most, cuts=(), kind=jnp.bfloat16):
    array = jax.random.normal(rng, shape, jnp.float32) * width
    if len(cuts) > 0:
        array = shard_levels(rng, shape, cuts, -0.22, 0.18) * array
    return jnp.clip(array, min=-most, max=most).astype(kind)


def setup_inputs(seed: int = 0) -> dict:
    arg_keys = jax.random.split(jax.random.key(seed), 9)
    p_start = draw_p_start(jax.random.fold_in(arg_keys[8], 71), 0)
    r_start = draw_r_start(jax.random.fold_in(arg_keys[8], 71), 0)
    diag_shift = jnp.clip(jnp.exp(math.log(2.0) - 1.3862944 * jax.random.uniform(arg_keys[2], (NBLK, BS), jnp.float32) ** shard_levels(arg_keys[2], (NBLK, BS), ((0, 128),), -0.2, 0.2)), 0.5, 2.0)
    shifts = jnp.clip(jax.random.uniform(arg_keys[3], (S,), jnp.float32, 0.5, 1.5), 0.5, 1.5)
    block_values = bell_draw(arg_keys[4], (NBLK, NB, BS, BS), (NB * BS) ** -0.5, 0.21875, ((0, 128),), jnp.float32)
    block_cols = draw_block_cols(jax.random.fold_in(arg_keys[8], 71), 0)
    live_slots = draw_live_slots(jax.random.fold_in(arg_keys[8], 71), 0)
    needed = place_ends(jax.random.randint(arg_keys[7], (N_GROUP * N_DOM, 4, HALO), 0, BR_DEV), jax.random.fold_in(arg_keys[7], 1), 0, BR_DEV - 1).astype(jnp.int32)
    return dict(p_start=p_start, r_start=r_start, diag_shift=diag_shift, shifts=shifts, block_values=block_values, block_cols=block_cols, live_slots=live_slots, needed=needed)


def reference(p_start, r_start, diag_shift, shifts, block_values, block_cols, live_slots, needed):
    ndev = N_GROUP * N_DOM
    device_ids = jnp.arange(ndev, dtype=jnp.int32)
    group_ids = device_ids // N_DOM
    dom_ids = device_ids % N_DOM
    sources = [
        group_ids * N_DOM + jnp.maximum(dom_ids - 1, 0),
        group_ids * N_DOM + jnp.minimum(dom_ids + 1, N_DOM - 1),
        ((group_ids - 1) % N_GROUP) * N_DOM + dom_ids,
        ((group_ids + 1) % N_GROUP) * N_DOM + dom_ids,
    ]
    valid = [
        (dom_ids > 0).astype(jnp.float32),
        (dom_ids < N_DOM - 1).astype(jnp.float32),
        jnp.ones((ndev,), jnp.float32),
        jnp.ones((ndev,), jnp.float32),
    ]
    values = block_values.reshape(ndev, BR_DEV, NB, BS, BS)
    columns = block_cols.reshape(ndev, BR_DEV, NB)
    slot_ids = lax.broadcasted_iota(jnp.int32, (NBLK, NB), 1)
    masks = (slot_ids < live_slots[:, None]).astype(jnp.float32).reshape(ndev, BR_DEV, NB)

    def multiply(vector):
        blocks = vector.reshape(ndev, BR_DEV, BS)
        pieces = [blocks]
        for k in range(4):
            pieces.append(blocks[sources[k][:, None], needed[:, k, :]] * valid[k][:, None, None])
        extended = jnp.concatenate(pieces, axis=1)

        def single(item):
            vals, cols, live, ext = item
            picked = ext[cols] * live[:, :, None]
            return jnp.einsum("bsij,bsj->bi", vals, picked, precision=lax.Precision.HIGHEST)

        return lax.map(single, (values, columns, masks, extended)).reshape(NBLK, BS)

    def advance(vector, theta):
        return multiply(vector) + (diag_shift - theta) * vector

    p_fields = [p_start]
    for step in range(1, S + 1):
        p_fields.append(advance(p_fields[-1], shifts[step - 1]))
    r_fields = [r_start]
    for step in range(1, S):
        r_fields.append(advance(r_fields[-1], shifts[step - 1]))
    basis = jnp.stack(p_fields + r_fields)
    gram = jnp.einsum("kbi,lbi->kl", basis, basis, precision=lax.Precision.HIGHEST) / (NBLK * BS)
    return basis, gram
```

```python
import functools

import jax
import jax.numpy as jnp
from jax import lax
from jax.experimental import pallas as pl
from jax.experimental.pallas import tpu as pltpu
from jax.sharding import PartitionSpec as P

MESH = pl.DeviceIdType.MESH
UNROLL = 4
GROWS = 24


def split(x):
    high = x.astype(jnp.bfloat16)
    low = (x - high.astype(jnp.float32)).astype(jnp.bfloat16)
    return high, low


def kernel(
    rows, slots, bs, halo, depth, n_group, n_dom,
    p_hbm, r_hbm, diag_hbm, shifts, values_hbm, cols, live, needed,
    basis_hbm, gram_hbm,
    stage, weights, ext_a, ext_b, fields, out, start, diag, index,
    gram_mine, gram_in_a, gram_in_b, gram_in_c, gram_out,
    value_sem, small_sem, out_sem, send_sem, recv_sem, gram_send, gram_recv,
):
    g = lax.axis_index("group")
    m = lax.axis_index("dom")
    column = 8
    n_x = n_dom // column
    x, w = m // column, m % column

    def dom_peer(i):
        return (g, i)

    small = [
        pltpu.make_async_copy(p_hbm, start.at[0], small_sem.at[0]),
        pltpu.make_async_copy(r_hbm, start.at[1], small_sem.at[1]),
        pltpu.make_async_copy(diag_hbm, diag, small_sem.at[2]),
    ]
    for copy in small:
        copy.start()

    def value_copy(b):
        return pltpu.make_async_copy(values_hbm.at[b], stage.at[b], value_sem.at[b])

    def start_values(b, carry):
        value_copy(b).start()
        return carry

    lax.fori_loop(0, rows, start_values, 0)

    neighbours = (
        (g, (m + n_dom - 1) % n_dom),
        (g, (m + 1) % n_dom),
        ((g + n_group - 1) % n_group, m),
        ((g + 1) % n_group, m),
    )
    peers_a = [dom_peer(x * column + (w + j) % column) for j in range(1, column)]
    peers_b = [dom_peer((x + j) % n_x * column + w) for j in range(1, n_x)]
    peers_c = [((g + j) % n_group, m) for j in range(1, n_group)]
    greeted = list(neighbours[:2]) + peers_a + peers_b + peers_c
    barrier = pltpu.get_barrier_semaphore()
    for peer in greeted:
        pl.semaphore_signal(barrier, inc=1, device_id=peer, device_id_type=MESH)

    for copy in small:
        copy.wait()
    width = 2 * rows
    for ext in (ext_a, ext_b):
        ext[5 * width : 5 * width + 16, :] = jnp.zeros((16, bs), jnp.float32)
    ext_a[pl.ds(0, rows, stride=2), :] = start[0]
    ext_a[pl.ds(1, rows, stride=2), :] = start[1]
    pl.semaphore_wait(barrier, len(greeted))

    def field_copies(ext, parity):
        return [
            pltpu.make_async_remote_copy(
                src_ref=ext.at[0:width],
                dst_ref=ext.at[(1 + (k ^ 1)) * width : (2 + (k ^ 1)) * width],
                send_sem=send_sem.at[4 * parity + k],
                recv_sem=recv_sem.at[4 * parity + (k ^ 1)],
                device_id=neighbours[k],
                device_id_type=MESH,
            )
            for k in range(4)
        ]

    for copy in field_copies(ext_a, 0):
        copy.start()

    fields[...] = jnp.zeros(fields.shape, jnp.float32)
    out[0] = start[0]
    out[depth + 1] = start[1]

    def prepare(b, carry):
        value_copy(b).wait()
        for s in range(slots):
            high, low = split(stage[b, s].T)
            weights[b, s * bs : (s + 1) * bs, 0:bs] = high
            weights[b, s * bs : (s + 1) * bs, bs : 2 * bs] = low
        used = live[b]
        for s in range(slots):
            c = cols[b, s]
            far = jnp.maximum(c - rows, 0)
            k, h = far // halo, far % halo
            spot = jnp.where(c < rows, c, (1 + k) * rows + needed[0, k, h])
            index[b * slots + s] = jnp.where(s < used, 2 * spot, 5 * width)
        fields[b, 0:1, :] = start[0, pl.ds(b, 1), :]
        fields[b, depth + 1 : depth + 2, :] = start[1, pl.ds(b, 1), :]
        return carry

    lax.fori_loop(0, rows, prepare, 0)

    def advance(src, dst, step):
        theta = shifts[step - 1]

        def some(i, carry):
            for u in range(UNROLL):
                b = i * UNROLL + u
                parts = []
                for s in range(slots):
                    picked = src[pl.ds(index[b * slots + s], 8), :]
                    high, low = split(picked)
                    parts.append(jnp.concatenate([high, low], axis=0))
                lhs = jnp.concatenate(parts, axis=1)
                y = jnp.dot(lhs, weights[b], preferred_element_type=jnp.float32)
                y = (y[8:16, bs:] + y[8:16, :bs]) + (y[0:8, bs:] + y[0:8, :bs])
                own = src[pl.ds(2 * b, 2), :]
                new = y[0:2] + (diag[pl.ds(b, 1), :] - theta) * own
                dst[pl.ds(2 * b, 2), :] = new
                fields[b, pl.ds(step, 1), :] = new[0:1]
                r_row = jnp.where(step < depth, depth + 1 + step, GROWS - 1)
                fields[b, pl.ds(r_row, 1), :] = new[1:2]
            return carry

        lax.fori_loop(0, rows // UNROLL, some, 0)

    def finish(copies):
        for copy in copies:
            copy.wait_send()

    def pair(i, carry):
        for copy in field_copies(ext_a, 0):
            copy.wait()
        advance(ext_a, ext_b, 2 * i + 1)
        for copy in field_copies(ext_b, 1):
            copy.start()
        out[2 * i + 1] = ext_b[pl.ds(0, rows, stride=2), :]
        out[depth + 1 + 2 * i + 1] = ext_b[pl.ds(1, rows, stride=2), :]
        for copy in field_copies(ext_b, 1):
            copy.wait()
        advance(ext_b, ext_a, 2 * i + 2)

        @pl.when(i < depth // 2 - 1)
        def _():
            for copy in field_copies(ext_a, 0):
                copy.start()
            out[depth + 1 + 2 * i + 2] = ext_a[pl.ds(1, rows, stride=2), :]

        out[2 * i + 2] = ext_a[pl.ds(0, rows, stride=2), :]
        return carry

    lax.fori_loop(0, depth // 2, pair, 0)

    basis_copy = pltpu.make_async_copy(out, basis_hbm, out_sem.at[0])
    basis_copy.start()

    highs, lows = [], []
    for b in range(rows):
        high, low = split(fields[b])
        highs.append(high)
        lows.append(low)
    both = jnp.concatenate(
        [jnp.concatenate(highs, axis=1), jnp.concatenate(lows, axis=1)], axis=0
    )
    prod = lax.dot_general(
        both, both, (((1,), (1,)), ((), ())), preferred_element_type=jnp.float32
    )
    gram = (prod[GROWS:, GROWS:] + prod[GROWS:, :GROWS]) + (prod[:GROWS, GROWS:] + prod[:GROWS, :GROWS])
    gram_mine[0] = jnp.zeros((GROWS, bs), jnp.float32)
    gram_mine[0, :, 0:GROWS] = gram

    phases = (
        (peers_a, column, w, gram_in_a, 0),
        (peers_b, n_x, x, gram_in_b, column),
        (peers_c, n_group, g, gram_in_c, column + n_x),
    )
    total = None
    for number, (peers, count, mine, landing, first) in enumerate(phases):
        copies = [
            pltpu.make_async_remote_copy(
                src_ref=gram_mine.at[number],
                dst_ref=landing.at[mine],
                send_sem=gram_send.at[first + j],
                recv_sem=gram_recv.at[first + j],
                device_id=peer,
                device_id_type=MESH,
            )
            for j, peer in enumerate(peers)
        ]
        for copy in copies:
            copy.start()
        landing[mine] = gram_mine[number]
        for copy in copies:
            copy.wait()
        total = landing[0]
        for i in range(1, count):
            total = total + landing[i]
        if number < 2:
            gram_mine[number + 1] = total
    cells = rows * bs * n_group * n_dom
    gram_out[...] = total * (1.0 / cells)
    gram_copy = pltpu.make_async_copy(gram_out, gram_hbm, out_sem.at[1])
    gram_copy.start()
    gram_copy.wait()
    basis_copy.wait()


def per_device(n_group, n_dom, p_start, r_start, diag_shift, shifts, block_values, block_cols, live_slots, needed):
    rows, bs = p_start.shape
    slots = block_cols.shape[1]
    halo = needed.shape[2]
    depth = shifts.shape[0]
    ncols = 2 * depth + 1
    f32 = jnp.float32
    hbm = pl.BlockSpec(memory_space=pl.ANY)
    smem = pl.BlockSpec(memory_space=pltpu.SMEM)
    dma = pltpu.SemaphoreType.DMA
    basis, gram = pl.pallas_call(
        functools.partial(kernel, rows, slots, bs, halo, depth, n_group, n_dom),
        out_shape=(
            jax.ShapeDtypeStruct((ncols, rows, bs), f32),
            jax.ShapeDtypeStruct((GROWS, bs), f32),
        ),
        in_specs=[hbm, hbm, hbm, smem, hbm, smem, smem, smem],
        out_specs=(hbm, hbm),
        scratch_shapes=[
            pltpu.VMEM((rows, slots, bs, bs), f32),
            pltpu.VMEM((rows, slots * bs, 2 * bs), jnp.bfloat16),
            pltpu.VMEM((10 * rows + 16, bs), f32),
            pltpu.VMEM((10 * rows + 16, bs), f32),
            pltpu.VMEM((rows, GROWS, bs), f32),
            pltpu.VMEM((ncols, rows, bs), f32),
            pltpu.VMEM((2, rows, bs), f32),
            pltpu.VMEM((rows, bs), f32),
            pltpu.SMEM((rows * slots,), jnp.int32),
            pltpu.VMEM((3, GROWS, bs), f32),
            pltpu.VMEM((8, GROWS, bs), f32),
            pltpu.VMEM((n_dom // 8, GROWS, bs), f32),
            pltpu.VMEM((n_group, GROWS, bs), f32),
            pltpu.VMEM((GROWS, bs), f32),
            dma((rows,)),
            dma((3,)),
            dma((2,)),
            dma((8,)),
            dma((8,)),
            dma((16,)),
            dma((16,)),
        ],
        compiler_params=pltpu.CompilerParams(
            collective_id=0, has_side_effects=True, vmem_limit_bytes=60 * 1024 * 1024
        ),
    )(p_start, r_start, diag_shift, shifts, block_values, block_cols, live_slots, needed)
    return basis, gram[:ncols, :ncols]


def solution(mesh):
    both = ("group", "dom")
    in_specs = (
        P(both, None),
        P(both, None),
        P(both, None),
        P(),
        P(both, None, None, None),
        P(both, None),
        P(both),
        P(both, None, None),
    )
    return jax.shard_map(
        functools.partial(per_device, mesh.shape["group"], mesh.shape["dom"]),
        mesh=mesh,
        in_specs=in_specs,
        out_specs=(P(None, both, None), P()),
        check_vma=False,
    )
```

```python
import functools

import jax
import jax.numpy as jnp
from jax import lax
from jax.experimental import pallas as pl
from jax.experimental.pallas import tpu as pltpu
from jax.sharding import PartitionSpec as P

MESH = pl.DeviceIdType.MESH
UNROLL = 32
GROWS = 24
COLUMN = 8


def split(x):
    high = x.astype(jnp.bfloat16)
    low = (x - high.astype(jnp.float32)).astype(jnp.bfloat16)
    return high, low


def both_halves(x):
    high, low = split(x)
    return jnp.concatenate([high, low], axis=0)


def four_sum(y, bs):
    return (y[8:16, bs:] + y[8:16, :bs]) + (y[0:8, bs:] + y[0:8, :bs])


def kernel(
    rows, slots, bs, halo, depth, n_group, n_dom,
    p_hbm, r_hbm, diag_hbm, shifts, values_hbm, cols, live, needed,
    basis_hbm, gram_hbm,
    stage, weights, ext_a, ext_b, fields, out, start, diag, index, partial,
    gram_mine, gram_in_a, gram_in_b, gram_out,
    value_sem, small_sem, out_sem, send_sem, recv_sem, gram_send, gram_recv,
):
    g = lax.axis_index("group")
    m = lax.axis_index("dom")
    n_x = n_dom // COLUMN
    x, w = m // COLUMN, m % COLUMN
    width = 2 * rows
    nothing = 5 * width

    small = [
        pltpu.make_async_copy(p_hbm, start.at[0], small_sem.at[0]),
        pltpu.make_async_copy(r_hbm, start.at[1], small_sem.at[1]),
        pltpu.make_async_copy(diag_hbm, diag, small_sem.at[2]),
    ]
    for copy in small:
        copy.start()

    neighbours = (
        (g, (m + n_dom - 1) % n_dom),
        (g, (m + 1) % n_dom),
        ((g + n_group - 1) % n_group, m),
        ((g + 1) % n_group, m),
    )
    peers_a = [(g, x * COLUMN + (w + j) % COLUMN) for j in range(1, COLUMN)]
    peers_b = [
        ((g + j // n_x) % n_group, (x + j) % n_x * COLUMN + w) for j in range(1, n_x * n_group)
    ]
    greeted = list(neighbours[:2]) + peers_a + peers_b
    barrier = pltpu.get_barrier_semaphore()
    for peer in greeted:
        pl.semaphore_signal(barrier, inc=1, device_id=peer, device_id_type=MESH)

    def value_copy(b):
        return pltpu.make_async_copy(values_hbm.at[b], stage.at[b], value_sem.at[b])

    def start_values(b, carry):
        value_copy(b).start()
        return carry

    lax.fori_loop(0, rows, start_values, 0)

    for copy in small:
        copy.wait()
    for ext in (ext_a, ext_b):
        ext[nothing : nothing + 16, :] = jnp.zeros((16, bs), jnp.float32)
    ext_a[pl.ds(0, rows, stride=2), :] = start[0]
    ext_a[pl.ds(1, rows, stride=2), :] = start[1]
    fields[...] = jnp.zeros(fields.shape, jnp.float32)

    def field_copies(ext, parity):
        return [
            pltpu.make_async_remote_copy(
                src_ref=ext.at[0:width],
                dst_ref=ext.at[(1 + (k ^ 1)) * width : (2 + (k ^ 1)) * width],
                send_sem=send_sem.at[4 * parity + k],
                recv_sem=recv_sem.at[4 * parity + (k ^ 1)],
                device_id=neighbours[k],
                device_id_type=MESH,
            )
            for k in range(4)
        ]

    def prepare(b, carry):
        value_copy(b).wait()
        for s in range(slots):
            high, low = split(stage[b, s].T)
            weights[b, 0, s * bs : (s + 1) * bs, :] = high
            weights[b, 1, s * bs : (s + 1) * bs, :] = low
        used = live[b]
        for s in range(1, slots):
            c = cols[s, b]
            far = jnp.maximum(c - rows, 0)
            k, h = far // halo, far % halo
            spot = jnp.where(c < rows, c, (1 + k) * rows + needed[0, k, h])
            index[b * slots + s] = jnp.where(s < used, 2 * spot, nothing)
        return carry

    lax.fori_loop(0, rows // 2, prepare, 0)
    pl.semaphore_wait(barrier, len(greeted))
    for copy in field_copies(ext_a, 0):
        copy.start()
    lax.fori_loop(rows // 2, rows, prepare, 0)

    def matrix(b, first, last):
        span = slice(first * bs, last * bs)
        return jnp.concatenate([weights[b, 0, span, :], weights[b, 1, span, :]], axis=1)

    def keep(src, step):
        out[step] = src[pl.ds(0, rows, stride=2), :]
        r_row = jnp.where(step < depth, depth + 1 + step, GROWS - 1)

        @pl.when(step < depth)
        def _():
            out[depth + 1 + step] = src[pl.ds(1, rows, stride=2), :]

        for b in range(rows):
            fields[b, pl.ds(step, 1), :] = src[2 * b : 2 * b + 1, :]
            fields[b, pl.ds(r_row, 1), :] = src[2 * b + 1 : 2 * b + 2, :]

    def ahead(src, step):
        theta = shifts[step]
        for first in range(0, rows, 4):
            own = src[2 * first : 2 * first + 8, :]
            lhs = both_halves(own)
            for j in range(4):
                b, two = first + j, slice(2 * j, 2 * j + 2)
                y = jnp.dot(lhs, matrix(b, 0, 1), preferred_element_type=jnp.float32)
                near = four_sum(y, bs)[two] + (diag[b : b + 1, :] - theta) * own[two]
                partial[2 * b : 2 * b + 2, :] = near

    def advance(src, dst):
        def some(i, carry):
            for u in range(UNROLL):
                b = i * UNROLL + u
                lhs = jnp.concatenate(
                    [
                        both_halves(src[pl.ds(index[b * slots + s], 8), :])
                        for s in range(1, slots)
                    ],
                    axis=1,
                )
                y = jnp.dot(lhs, matrix(b, 1, slots), preferred_element_type=jnp.float32)
                dst[pl.ds(2 * b, 2), :] = four_sum(y, bs)[0:2] + partial[pl.ds(2 * b, 2), :]
            return carry

        lax.fori_loop(0, rows // UNROLL, some, 0)

    ahead(ext_a, 0)
    keep(ext_a, 0)

    def pair(i, carry):
        for copy in field_copies(ext_a, 0):
            copy.wait()
        advance(ext_a, ext_b)
        for copy in field_copies(ext_b, 1):
            copy.start()
        ahead(ext_b, 2 * i + 1)
        keep(ext_b, 2 * i + 1)
        for copy in field_copies(ext_b, 1):
            copy.wait()
        advance(ext_b, ext_a)

        @pl.when(i < depth // 2 - 1)
        def _():
            for copy in field_copies(ext_a, 0):
                copy.start()
            ahead(ext_a, 2 * i + 2)

        keep(ext_a, 2 * i + 2)
        return carry

    lax.fori_loop(0, depth // 2, pair, 0)

    basis_copy = pltpu.make_async_copy(out, basis_hbm, out_sem.at[0])
    basis_copy.start()

    highs, lows = [], []
    for b in range(rows):
        high, low = split(fields[b])
        highs.append(high)
        lows.append(low)
    both = jnp.concatenate(
        [jnp.concatenate(highs, axis=1), jnp.concatenate(lows, axis=1)], axis=0
    )
    prod = lax.dot_general(
        both, both, (((1,), (1,)), ((), ())), preferred_element_type=jnp.float32
    )
    gram = (prod[GROWS:, GROWS:] + prod[GROWS:, :GROWS]) + (
        prod[:GROWS, GROWS:] + prod[:GROWS, :GROWS]
    )
    gram_mine[0] = jnp.zeros((8, bs), jnp.float32)
    for i in range(GROWS // 8):
        gram_mine[0, :, 32 * i : 32 * i + GROWS] = gram[8 * i : 8 * i + 8]

    phases = (
        (peers_a, COLUMN, w, gram_in_a, 0),
        (peers_b, n_x * n_group, g * n_x + x, gram_in_b, COLUMN),
    )
    total = None
    for number, (peers, count, mine, landing, first) in enumerate(phases):
        copies = [
            pltpu.make_async_remote_copy(
                src_ref=gram_mine.at[number],
                dst_ref=landing.at[mine],
                send_sem=gram_send.at[first + j],
                recv_sem=gram_recv.at[first + j],
                device_id=peer,
                device_id_type=MESH,
            )
            for j, peer in enumerate(peers)
        ]
        for copy in copies:
            copy.start()
        landing[mine] = gram_mine[number]
        for copy in copies:
            copy.wait()
        total = landing[0]
        for i in range(1, count):
            total = total + landing[i]
        if number < 1:
            gram_mine[number + 1] = total
    total = total * (1.0 / (rows * bs * n_group * n_dom))
    gram_out[...] = jnp.zeros((GROWS, bs), jnp.float32)
    for i in range(GROWS // 8):
        gram_out[8 * i : 8 * i + 8, 0:GROWS] = total[:, 32 * i : 32 * i + GROWS]
    gram_copy = pltpu.make_async_copy(gram_out, gram_hbm, out_sem.at[1])
    gram_copy.start()
    gram_copy.wait()
    basis_copy.wait()


def per_device(n_group, n_dom, p_start, r_start, diag_shift, shifts, block_values, block_cols, live_slots, needed):
    rows, bs = p_start.shape
    slots = block_cols.shape[1]
    halo = needed.shape[2]
    depth = shifts.shape[0]
    ncols = 2 * depth + 1
    f32 = jnp.float32
    hbm = pl.BlockSpec(memory_space=pl.ANY)
    smem = pl.BlockSpec(memory_space=pltpu.SMEM)
    dma = pltpu.SemaphoreType.DMA
    peers_b = n_group * n_dom // COLUMN
    basis, gram = pl.pallas_call(
        functools.partial(kernel, rows, slots, bs, halo, depth, n_group, n_dom),
        out_shape=(
            jax.ShapeDtypeStruct((ncols, rows, bs), f32),
            jax.ShapeDtypeStruct((GROWS, bs), f32),
        ),
        in_specs=[hbm, hbm, hbm, smem, hbm, smem, smem, smem],
        out_specs=(hbm, hbm),
        scratch_shapes=[
            pltpu.VMEM((rows, slots, bs, bs), f32),
            pltpu.VMEM((rows, 2, slots * bs, bs), jnp.bfloat16),
            pltpu.VMEM((10 * rows + 16, bs), f32),
            pltpu.VMEM((10 * rows + 16, bs), f32),
            pltpu.VMEM((rows, GROWS, bs), f32),
            pltpu.VMEM((ncols, rows, bs), f32),
            pltpu.VMEM((2, rows, bs), f32),
            pltpu.VMEM((rows, bs), f32),
            pltpu.SMEM((rows * slots,), jnp.int32),
            pltpu.VMEM((2 * rows, bs), f32),
            pltpu.VMEM((2, 8, bs), f32),
            pltpu.VMEM((COLUMN, 8, bs), f32),
            pltpu.VMEM((peers_b, 8, bs), f32),
            pltpu.VMEM((GROWS, bs), f32),
            dma((rows,)),
            dma((3,)),
            dma((2,)),
            dma((8,)),
            dma((8,)),
            dma((COLUMN + peers_b,)),
            dma((COLUMN + peers_b,)),
        ],
        compiler_params=pltpu.CompilerParams(
            collective_id=0, has_side_effects=True, vmem_limit_bytes=60 * 1024 * 1024
        ),
    )(p_start, r_start, diag_shift, shifts, block_values, block_cols.T, live_slots, needed)
    return basis, gram[:ncols, :ncols]


def solution(mesh):
    both = ("group", "dom")
    in_specs = (
        P(both, None),
        P(both, None),
        P(both, None),
        P(),
        P(both, None, None, None),
        P(both, None),
        P(both),
        P(both, None, None),
    )
    return jax.shard_map(
        functools.partial(per_device, mesh.shape["group"], mesh.shape["dom"]),
        mesh=mesh,
        in_specs=in_specs,
        out_specs=(P(None, both, None), P()),
        check_vma=False,
    )
```

```python
import functools

import jax
import jax.numpy as jnp
from jax import lax
from jax.experimental import pallas as pl
from jax.experimental.pallas import tpu as pltpu
from jax.sharding import PartitionSpec as P

MESH = pl.DeviceIdType.MESH
UNROLL = 32
GROWS = 24
COLUMN = 8


def split(x):
    high = x.astype(jnp.bfloat16)
    low = (x - high.astype(jnp.float32)).astype(jnp.bfloat16)
    return high, low


def both_halves(x):
    high, low = split(x)
    return jnp.concatenate([high, low], axis=0)


def four_sum(y, bs):
    return (y[8:16, bs:] + y[8:16, :bs]) + (y[0:8, bs:] + y[0:8, :bs])


def kernel(
    rows, slots, bs, halo, depth, n_group, n_dom,
    p_hbm, r_hbm, diag_hbm, shifts_hbm, values_hbm, cols_hbm, live_hbm, needed_hbm,
    out, gram_out,
    shifts, cols, live, needed, stage, weights, ext_a, ext_b, fields, start, diag, index, partial,
    gram_mine, gram_in_a, gram_in_b,
    value_sem, small_sem, send_sem, recv_sem, gram_send, gram_recv,
):
    g = lax.axis_index("group")
    m = lax.axis_index("dom")
    n_x = n_dom // COLUMN
    x, w = m // COLUMN, m % COLUMN
    width = 2 * rows
    nothing = 5 * width

    small = [
        pltpu.make_async_copy(p_hbm, start.at[0], small_sem.at[0]),
        pltpu.make_async_copy(r_hbm, start.at[1], small_sem.at[1]),
        pltpu.make_async_copy(diag_hbm, diag, small_sem.at[2]),
        pltpu.make_async_copy(cols_hbm, cols, small_sem.at[3]),
        pltpu.make_async_copy(live_hbm, live, small_sem.at[4]),
        pltpu.make_async_copy(needed_hbm, needed, small_sem.at[5]),
        pltpu.make_async_copy(shifts_hbm, shifts, small_sem.at[6]),
    ]
    for copy in small:
        copy.start()

    neighbours = (
        (g, (m + n_dom - 1) % n_dom),
        (g, (m + 1) % n_dom),
        ((g + n_group - 1) % n_group, m),
        ((g + 1) % n_group, m),
    )
    peers_a = [(g, x * COLUMN + (w + j) % COLUMN) for j in range(1, COLUMN)]
    peers_b = [
        ((g + j // n_x) % n_group, (x + j) % n_x * COLUMN + w) for j in range(1, n_x * n_group)
    ]
    before, after = m > 0, m < n_dom - 1

    def where_there(k, act):
        if k < 2:
            pl.when((before, after)[k])(act)
        else:
            act()

    barrier = pltpu.get_barrier_semaphore()

    def greet(peer):
        pl.semaphore_signal(barrier, inc=1, device_id=peer, device_id_type=MESH)

    for k in range(2):
        where_there(k, functools.partial(greet, neighbours[k]))
    for peer in peers_a + peers_b:
        greet(peer)
    greetings = len(peers_a + peers_b) + before.astype(jnp.int32) + after.astype(jnp.int32)

    def value_copy(b):
        return pltpu.make_async_copy(values_hbm.at[b], stage.at[b], value_sem.at[b])

    def start_values(b, carry):
        value_copy(b).start()
        return carry

    lax.fori_loop(0, rows, start_values, 0)

    for copy in small:
        copy.wait()
    for ext in (ext_a, ext_b):
        ext[nothing : nothing + 16, :] = jnp.zeros((16, bs), jnp.float32)
    ext_a[pl.ds(0, rows, stride=2), :] = start[0]
    ext_a[pl.ds(1, rows, stride=2), :] = start[1]
    fields[...] = jnp.zeros(fields.shape, jnp.float32)

    def field_copy(ext, parity, k, landing):
        return pltpu.make_async_remote_copy(
            src_ref=ext.at[0:width],
            dst_ref=ext.at[(1 + landing) * width : (2 + landing) * width],
            send_sem=send_sem.at[4 * parity + k],
            recv_sem=recv_sem.at[4 * parity + landing],
            device_id=neighbours[k],
            device_id_type=MESH,
        )

    def send_field(ext, parity):
        for k in range(4):
            where_there(k, field_copy(ext, parity, k, k ^ 1).start)

    def await_field(ext, parity):
        for k in range(4):
            where_there(k, field_copy(ext, parity, k, k).wait_recv)
        for k in range(4):
            where_there(k, field_copy(ext, parity, k, k ^ 1).wait_send)

    def prepare(b, carry):
        value_copy(b).wait()
        for s in range(slots):
            high, low = split(stage[b, s].T)
            weights[b, 0, s * bs : (s + 1) * bs, :] = high
            weights[b, 1, s * bs : (s + 1) * bs, :] = low
        used = live[b]
        for s in range(1, slots):
            c = cols[s, b]
            far = jnp.maximum(c - rows, 0)
            k, h = far // halo, far % halo
            spot = jnp.where(c < rows, c, (1 + k) * rows + needed[0, k, h])
            index[b * slots + s] = jnp.where(s < used, 2 * spot, nothing)
        return carry

    lax.fori_loop(0, rows // 2, prepare, 0)
    pl.semaphore_wait(barrier, greetings)
    send_field(ext_a, 0)
    lax.fori_loop(rows // 2, rows, prepare, 0)

    def matrix(b, first, last):
        span = slice(first * bs, last * bs)
        return jnp.concatenate([weights[b, 0, span, :], weights[b, 1, span, :]], axis=1)

    def keep(src, step):
        out[step] = src[pl.ds(0, rows, stride=2), :]
        r_row = jnp.where(step < depth, depth + 1 + step, GROWS - 1)

        @pl.when(step < depth)
        def _():
            out[depth + 1 + step] = src[pl.ds(1, rows, stride=2), :]

        for b in range(rows):
            fields[b, pl.ds(step, 1), :] = src[2 * b : 2 * b + 1, :]
            fields[b, pl.ds(r_row, 1), :] = src[2 * b + 1 : 2 * b + 2, :]

    def ahead(src, step):
        theta = shifts[step]
        for first in range(0, rows, 4):
            own = src[2 * first : 2 * first + 8, :]
            lhs = both_halves(own)
            for j in range(4):
                b, two = first + j, slice(2 * j, 2 * j + 2)
                y = jnp.dot(lhs, matrix(b, 0, 1), preferred_element_type=jnp.float32)
                near = four_sum(y, bs)[two] + (diag[b : b + 1, :] - theta) * own[two]
                partial[2 * b : 2 * b + 2, :] = near

    def advance(src, dst):
        def some(i, carry):
            for u in range(UNROLL):
                b = i * UNROLL + u
                lhs = jnp.concatenate(
                    [
                        both_halves(src[pl.ds(index[b * slots + s], 8), :])
                        for s in range(1, slots)
                    ],
                    axis=1,
                )
                y = jnp.dot(lhs, matrix(b, 1, slots), preferred_element_type=jnp.float32)
                dst[pl.ds(2 * b, 2), :] = four_sum(y, bs)[0:2] + partial[pl.ds(2 * b, 2), :]
            return carry

        lax.fori_loop(0, rows // UNROLL, some, 0)

    ahead(ext_a, 0)
    keep(ext_a, 0)

    def pair(i, carry):
        await_field(ext_a, 0)
        advance(ext_a, ext_b)
        send_field(ext_b, 1)
        ahead(ext_b, 2 * i + 1)
        keep(ext_b, 2 * i + 1)
        await_field(ext_b, 1)
        advance(ext_b, ext_a)

        @pl.when(i < depth // 2 - 1)
        def _():
            send_field(ext_a, 0)
            ahead(ext_a, 2 * i + 2)

        keep(ext_a, 2 * i + 2)
        return carry

    lax.fori_loop(0, depth // 2, pair, 0)

    highs, lows = [], []
    for b in range(rows):
        high, low = split(fields[b])
        highs.append(high)
        lows.append(low)
    both = jnp.concatenate(
        [jnp.concatenate(highs, axis=1), jnp.concatenate(lows, axis=1)], axis=0
    )
    prod = lax.dot_general(
        both, both, (((1,), (1,)), ((), ())), preferred_element_type=jnp.float32
    )
    gram = (prod[GROWS:, GROWS:] + prod[GROWS:, :GROWS]) + (
        prod[:GROWS, GROWS:] + prod[:GROWS, :GROWS]
    )
    gram_mine[0] = jnp.zeros((8, bs), jnp.float32)
    for i in range(GROWS // 8):
        gram_mine[0, :, 32 * i : 32 * i + GROWS] = gram[8 * i : 8 * i + 8]

    phases = (
        (peers_a, COLUMN, w, gram_in_a, 0),
        (peers_b, n_x * n_group, g * n_x + x, gram_in_b, COLUMN),
    )
    total = None
    for number, (peers, count, mine, landing, first) in enumerate(phases):
        copies = [
            pltpu.make_async_remote_copy(
                src_ref=gram_mine.at[number],
                dst_ref=landing.at[mine],
                send_sem=gram_send.at[first + j],
                recv_sem=gram_recv.at[first + j],
                device_id=peer,
                device_id_type=MESH,
            )
            for j, peer in enumerate(peers)
        ]
        for copy in copies:
            copy.start()
        landing[mine] = gram_mine[number]
        for copy in copies:
            copy.wait()
        total = landing[0]
        for i in range(1, count):
            total = total + landing[i]
        if number < 1:
            gram_mine[number + 1] = total
    total = total * (1.0 / (rows * bs * n_group * n_dom))
    ncols = 2 * depth + 1
    for i in range(0, ncols, 8):
        some = min(8, ncols - i)
        gram_out[i : i + some, :] = total[0:some, 4 * i : 4 * i + ncols]


def deliver(basis, gram, basis_out, gram_out, sems):
    copies = [
        pltpu.make_async_copy(basis, basis_out, sems.at[0]),
        pltpu.make_async_copy(gram, gram_out, sems.at[1]),
    ]
    for copy in copies:
        copy.start()
    for copy in copies:
        copy.wait()


def per_device(n_group, n_dom, p_start, r_start, diag_shift, shifts, block_values, block_cols, live_slots, needed):
    rows, bs = p_start.shape
    slots = block_cols.shape[1]
    halo = needed.shape[2]
    depth = shifts.shape[0]
    ncols = 2 * depth + 1
    f32 = jnp.float32
    hbm = pl.BlockSpec(memory_space=pltpu.HBM)
    dma = pltpu.SemaphoreType.DMA
    peers_b = n_group * n_dom // COLUMN
    vmem = pl.BlockSpec(memory_space=pltpu.VMEM)
    results = (
        jax.ShapeDtypeStruct((ncols, rows, bs), f32),
        jax.ShapeDtypeStruct((ncols, ncols), f32),
    )
    basis, gram = pl.pallas_call(
        functools.partial(kernel, rows, slots, bs, halo, depth, n_group, n_dom),
        out_shape=tuple(pltpu.VMEM(r.shape, r.dtype) for r in results),
        in_specs=[hbm] * 8,
        out_specs=(vmem, vmem),
        scratch_shapes=[
            pltpu.SMEM((depth,), f32),
            pltpu.SMEM((slots, rows), jnp.int32),
            pltpu.SMEM((rows,), jnp.int32),
            pltpu.SMEM((1, 4, halo), jnp.int32),
            pltpu.VMEM((rows, slots, bs, bs), f32),
            pltpu.VMEM((rows, 2, slots * bs, bs), jnp.bfloat16),
            pltpu.VMEM((10 * rows + 16, bs), f32),
            pltpu.VMEM((10 * rows + 16, bs), f32),
            pltpu.VMEM((rows, GROWS, bs), f32),
            pltpu.VMEM((2, rows, bs), f32),
            pltpu.VMEM((rows, bs), f32),
            pltpu.SMEM((rows * slots,), jnp.int32),
            pltpu.VMEM((2 * rows, bs), f32),
            pltpu.VMEM((2, 8, bs), f32),
            pltpu.VMEM((COLUMN, 8, bs), f32),
            pltpu.VMEM((peers_b, 8, bs), f32),
            dma((rows,)),
            dma((7,)),
            dma((8,)),
            dma((8,)),
            dma((COLUMN + peers_b,)),
            dma((COLUMN + peers_b,)),
        ],
        compiler_params=pltpu.CompilerParams(
            collective_id=0, has_side_effects=True, vmem_limit_bytes=60 * 1024 * 1024
        ),
    )(p_start, r_start, diag_shift, shifts, block_values, block_cols.T, live_slots, needed)
    return pl.pallas_call(
        deliver,
        out_shape=results,
        in_specs=[vmem, vmem],
        out_specs=(hbm, hbm),
        scratch_shapes=[dma((2,))],
        compiler_params=pltpu.CompilerParams(vmem_limit_bytes=4 * 1024 * 1024),
    )(basis, gram)


def solution(mesh):
    both = ("group", "dom")
    in_specs = (
        P(both, None),
        P(both, None),
        P(both, None),
        P(),
        P(both, None, None, None),
        P(both, None),
        P(both),
        P(both, None, None),
    )
    return jax.shard_map(
        functools.partial(per_device, mesh.shape["group"], mesh.shape["dom"]),
        mesh=mesh,
        in_specs=in_specs,
        out_specs=(P(None, both, None), P()),
        check_vma=False,
    )
```

```python
import functools

import jax
import jax.numpy as jnp
from jax import lax
from jax.experimental import pallas as pl
from jax.experimental.pallas import tpu as pltpu
from jax.sharding import PartitionSpec as P

MESH = pl.DeviceIdType.MESH
UNROLL = 32
TOGETHER = 4
EARLY = 8
GROWS = 24
COLUMN = 8


def split(x):
    high = x.astype(jnp.bfloat16)
    low = (x - high.astype(jnp.float32)).astype(jnp.bfloat16)
    return high, low


def both_halves(x):
    high, low = split(x)
    return jnp.concatenate([high, low], axis=0)


def four_sum(y, bs):
    return (y[8:16, bs:] + y[8:16, :bs]) + (y[0:8, bs:] + y[0:8, :bs])


def kernel(
    rows, slots, bs, halo, depth, n_group, n_dom,
    p_hbm, r_hbm, diag_hbm, shifts_hbm, values_hbm, cols_hbm, live_hbm, needed_hbm,
    out, gram_out,
    shifts, cols, live, needed, stage, weights, ext_a, ext_b, fields, start, diag, index, partial,
    gram_mine, gram_in_a, gram_in_b, row_mine, row_in,
    value_sem, small_sem, send_sem, recv_sem, gram_send, gram_recv, row_send, row_recv,
):
    g = lax.axis_index("group")
    m = lax.axis_index("dom")
    n_x = n_dom // COLUMN
    x, w = m // COLUMN, m % COLUMN
    width = 2 * rows
    nothing = 5 * width

    small = [
        pltpu.make_async_copy(p_hbm, start.at[0], small_sem.at[0]),
        pltpu.make_async_copy(r_hbm, start.at[1], small_sem.at[1]),
        pltpu.make_async_copy(diag_hbm, diag, small_sem.at[2]),
        pltpu.make_async_copy(cols_hbm, cols, small_sem.at[3]),
        pltpu.make_async_copy(live_hbm, live, small_sem.at[4]),
        pltpu.make_async_copy(needed_hbm, needed, small_sem.at[5]),
        pltpu.make_async_copy(shifts_hbm, shifts, small_sem.at[6]),
    ]
    for copy in small:
        copy.start()

    neighbours = (
        (g, (m + n_dom - 1) % n_dom),
        (g, (m + 1) % n_dom),
        ((g + n_group - 1) % n_group, m),
        ((g + 1) % n_group, m),
    )
    peers_a = [(g, x * COLUMN + (w + j) % COLUMN) for j in range(1, COLUMN)]
    peers_b = [
        ((g + j // n_x) % n_group, (x + j) % n_x * COLUMN + w) for j in range(1, n_x * n_group)
    ]
    before, after = m > 0, m < n_dom - 1

    def where_there(k, act):
        if k < 2:
            pl.when((before, after)[k])(act)
        else:
            act()

    barrier = pltpu.get_barrier_semaphore()

    def greet(peer):
        pl.semaphore_signal(barrier, inc=1, device_id=peer, device_id_type=MESH)

    for k in range(2):
        where_there(k, functools.partial(greet, neighbours[k]))
    for peer in peers_a + peers_b:
        greet(peer)
    greetings = len(peers_a + peers_b) + before.astype(jnp.int32) + after.astype(jnp.int32)

    def value_copy(b):
        return pltpu.make_async_copy(values_hbm.at[b], stage.at[b], value_sem.at[b])

    def start_values(b, carry):
        value_copy(b).start()
        return carry

    lax.fori_loop(0, rows, start_values, 0)

    for copy in small:
        copy.wait()
    for ext in (ext_a, ext_b):
        ext[nothing : nothing + 16, :] = jnp.zeros((16, bs), jnp.float32)
    ext_a[pl.ds(0, rows, stride=2), :] = start[0]
    ext_a[pl.ds(1, rows, stride=2), :] = start[1]
    fields[...] = jnp.zeros(fields.shape, jnp.float32)

    def field_copy(ext, parity, k, landing):
        return pltpu.make_async_remote_copy(
            src_ref=ext.at[0:width],
            dst_ref=ext.at[(1 + landing) * width : (2 + landing) * width],
            send_sem=send_sem.at[4 * parity + k],
            recv_sem=recv_sem.at[4 * parity + landing],
            device_id=neighbours[k],
            device_id_type=MESH,
        )

    def send_field(ext, parity):
        for k in range(4):
            where_there(k, field_copy(ext, parity, k, k ^ 1).start)

    def await_field(ext, parity):
        for k in range(4):
            where_there(k, field_copy(ext, parity, k, k).wait_recv)
        for k in range(4):
            where_there(k, field_copy(ext, parity, k, k ^ 1).wait_send)

    def prepare_one(b):
        for s in range(slots):
            high, low = split(stage[b, s].T)
            weights[b, 0, s * bs : (s + 1) * bs, :] = high
            weights[b, 1, s * bs : (s + 1) * bs, :] = low
        used = live[b]
        for s in range(1, slots):
            c = cols[s, b]
            far = jnp.maximum(c - rows, 0)
            k, h = far // halo, far % halo
            spot = jnp.where(c < rows, c, (1 + k) * rows + needed[0, k, h])
            index[b * slots + s] = jnp.where(s < used, 2 * spot, nothing)

    def prepare(i, carry):
        for u in range(TOGETHER):
            value_copy(i * TOGETHER + u).wait()
        for u in range(TOGETHER):
            prepare_one(i * TOGETHER + u)
        return carry

    lax.fori_loop(0, EARLY // TOGETHER, prepare, 0)
    pl.semaphore_wait(barrier, greetings)
    send_field(ext_a, 0)
    lax.fori_loop(EARLY // TOGETHER, rows // TOGETHER, prepare, 0)

    def matrix(b, first, last):
        span = slice(first * bs, last * bs)
        return jnp.concatenate([weights[b, 0, span, :], weights[b, 1, span, :]], axis=1)

    def keep(src, step):
        out[step] = src[pl.ds(0, rows, stride=2), :]
        r_row = jnp.where(step < depth, depth + 1 + step, GROWS - 1)

        @pl.when(step < depth)
        def _():
            out[depth + 1 + step] = src[pl.ds(1, rows, stride=2), :]

        for b in range(rows):
            fields[b, pl.ds(step, 1), :] = src[2 * b : 2 * b + 1, :]
            fields[b, pl.ds(r_row, 1), :] = src[2 * b + 1 : 2 * b + 2, :]

    def ahead(src, step):
        theta = shifts[step]
        for first in range(0, rows, 4):
            own = src[2 * first : 2 * first + 8, :]
            lhs = both_halves(own)
            for j in range(4):
                b, two = first + j, slice(2 * j, 2 * j + 2)
                y = jnp.dot(lhs, matrix(b, 0, 1), preferred_element_type=jnp.float32)
                near = four_sum(y, bs)[two] + (diag[b : b + 1, :] - theta) * own[two]
                partial[2 * b : 2 * b + 2, :] = near

    def advance(src, dst):
        def some(i, carry):
            for u in range(UNROLL):
                b = i * UNROLL + u
                lhs = jnp.concatenate(
                    [
                        both_halves(src[pl.ds(index[b * slots + s], 8), :])
                        for s in range(1, slots)
                    ],
                    axis=1,
                )
                y = jnp.dot(lhs, matrix(b, 1, slots), preferred_element_type=jnp.float32)
                dst[pl.ds(2 * b, 2), :] = four_sum(y, bs)[0:2] + partial[pl.ds(2 * b, 2), :]
            return carry

        lax.fori_loop(0, rows // UNROLL, some, 0)

    def gram_part():
        highs, lows = [], []
        for b in range(rows):
            high, low = split(fields[b])
            highs.append(high)
            lows.append(low)
        both = jnp.concatenate(
            [jnp.concatenate(highs, axis=1), jnp.concatenate(lows, axis=1)], axis=0
        )
        prod = lax.dot_general(
            both, both, (((1,), (1,)), ((), ())), preferred_element_type=jnp.float32
        )
        gram = (prod[GROWS:, GROWS:] + prod[GROWS:, :GROWS]) + (
            prod[:GROWS, GROWS:] + prod[:GROWS, :GROWS]
        )
        gram_mine[0] = jnp.zeros((8, bs), jnp.float32)
        for i in range(GROWS // 8):
            gram_mine[0, :, 32 * i : 32 * i + GROWS] = gram[8 * i : 8 * i + 8]

    rounds = (
        (peers_a, w, gram_in_a, 0),
        (peers_b, g * n_x + x, gram_in_b, COLUMN),
    )

    def round_copies(number):
        peers, mine, landing, first = rounds[number]
        return [
            pltpu.make_async_remote_copy(
                src_ref=gram_mine.at[number],
                dst_ref=landing.at[mine],
                send_sem=gram_send.at[first + j],
                recv_sem=gram_recv.at[first + j],
                device_id=peer,
                device_id_type=MESH,
            )
            for j, peer in enumerate(peers)
        ]

    def start_round(number):
        _, mine, landing, _ = rounds[number]
        for copy in round_copies(number):
            copy.start()
        landing[mine] = gram_mine[number]

    def end_round(number):
        peers, _, landing, _ = rounds[number]
        for copy in round_copies(number):
            copy.wait()
        total = landing[0]
        for i in range(1, len(peers) + 1):
            total = total + landing[i]
        return total

    ahead(ext_a, 0)
    keep(ext_a, 0)

    def pair(i, carry):
        await_field(ext_a, 0)
        advance(ext_a, ext_b)
        send_field(ext_b, 1)
        ahead(ext_b, 2 * i + 1)
        keep(ext_b, 2 * i + 1)

        @pl.when(i == depth // 2 - 1)
        def _():
            gram_part()
            start_round(0)

        await_field(ext_b, 1)
        advance(ext_b, ext_a)

        @pl.when(i < depth // 2 - 1)
        def _():
            send_field(ext_a, 0)
            ahead(ext_a, 2 * i + 2)

        keep(ext_a, 2 * i + 2)
        return carry

    lax.fori_loop(0, depth // 2, pair, 0)

    last = jnp.zeros((GROWS, bs), jnp.float32)
    for b in range(rows):
        last = last + fields[b] * ext_a[2 * b : 2 * b + 1, :]
    row_mine[...] = jnp.zeros((1, bs), jnp.float32)
    row_mine[:, 0:GROWS] = jnp.sum(last.T, axis=0, keepdims=True)
    count = n_group * n_dom
    me = g * n_dom + m

    def hops(offset, size):
        return min(offset, size - offset)

    offsets = sorted(
        ((dg, dx) for dg in range(n_group) for dx in range(n_x)),
        key=lambda o: -(hops(o[0], n_group) + hops(o[1], n_x)),
    )
    for dg, dx in offsets:

        def send_row(j, carry, to_g=(g + dg) % n_group, to_x=(x + dx) % n_x):
            pltpu.make_async_remote_copy(
                src_ref=row_mine,
                dst_ref=row_in.at[me],
                send_sem=row_send.at[0],
                recv_sem=row_recv.at[0],
                device_id=(to_g, to_x * COLUMN + (w + j) % COLUMN),
                device_id_type=MESH,
            ).start()
            return carry

        for j in range(0 if dg or dx else 1, COLUMN):
            send_row(j, 0)
    row_in[me] = row_mine[...]

    gram_mine[1] = end_round(0)
    start_round(1)
    total = end_round(1)

    rows_sent = pltpu.make_async_remote_copy(
        src_ref=row_in.at[0 : count - 1],
        dst_ref=row_in.at[0 : count - 1],
        send_sem=row_send.at[0],
        recv_sem=row_recv.at[0],
        device_id=neighbours[3],
        device_id_type=MESH,
    )
    rows_sent.wait_recv()
    rows_sent.wait_send()
    row = row_in[0]
    for i in range(1, count):
        row = row + row_in[i]

    scale = 1.0 / (rows * bs * count)
    ncols = 2 * depth + 1
    across = jnp.broadcast_to(row, (bs, bs))
    down = across.T
    for i in range(0, ncols, 8):
        some = min(8, ncols - i)
        part = total[0:some, 4 * i : 4 * i + ncols]
        r = i + lax.broadcasted_iota(jnp.int32, (some, ncols), 0)
        c = lax.broadcasted_iota(jnp.int32, (some, ncols), 1)
        part = jnp.where(c == depth, down[i : i + some, 0:ncols], part)
        part = jnp.where(r == depth, across[i : i + some, 0:ncols], part)
        gram_out[i : i + some, :] = part * scale


def deliver(basis, gram, basis_out, gram_out, sems):
    copies = [
        pltpu.make_async_copy(basis, basis_out, sems.at[0]),
        pltpu.make_async_copy(gram, gram_out, sems.at[1]),
    ]
    for copy in copies:
        copy.start()
    for copy in copies:
        copy.wait()


def per_device(n_group, n_dom, p_start, r_start, diag_shift, shifts, block_values, block_cols, live_slots, needed):
    rows, bs = p_start.shape
    slots = block_cols.shape[1]
    halo = needed.shape[2]
    depth = shifts.shape[0]
    ncols = 2 * depth + 1
    f32 = jnp.float32
    hbm = pl.BlockSpec(memory_space=pltpu.HBM)
    dma = pltpu.SemaphoreType.DMA
    peers_b = n_group * n_dom // COLUMN
    vmem = pl.BlockSpec(memory_space=pltpu.VMEM)
    results = (
        jax.ShapeDtypeStruct((ncols, rows, bs), f32),
        jax.ShapeDtypeStruct((ncols, ncols), f32),
    )
    basis, gram = pl.pallas_call(
        functools.partial(kernel, rows, slots, bs, halo, depth, n_group, n_dom),
        out_shape=tuple(pltpu.VMEM(r.shape, r.dtype) for r in results),
        in_specs=[hbm] * 8,
        out_specs=(vmem, vmem),
        scratch_shapes=[
            pltpu.SMEM((depth,), f32),
            pltpu.SMEM((slots, rows), jnp.int32),
            pltpu.SMEM((rows,), jnp.int32),
            pltpu.SMEM((1, 4, halo), jnp.int32),
            pltpu.VMEM((rows, slots, bs, bs), f32),
            pltpu.VMEM((rows, 2, slots * bs, bs), jnp.bfloat16),
            pltpu.VMEM((10 * rows + 16, bs), f32),
            pltpu.VMEM((10 * rows + 16, bs), f32),
            pltpu.VMEM((rows, GROWS, bs), f32),
            pltpu.VMEM((2, rows, bs), f32),
            pltpu.VMEM((rows, bs), f32),
            pltpu.SMEM((rows * slots,), jnp.int32),
            pltpu.VMEM((2 * rows, bs), f32),
            pltpu.VMEM((2, 8, bs), f32),
            pltpu.VMEM((COLUMN, 8, bs), f32),
            pltpu.VMEM((peers_b, 8, bs), f32),
            pltpu.VMEM((1, bs), f32),
            pltpu.VMEM((n_group * n_dom, 1, bs), f32),
            dma((rows,)),
            dma((7,)),
            dma((8,)),
            dma((8,)),
            dma((COLUMN + peers_b,)),
            dma((COLUMN + peers_b,)),
            dma((1,)),
            dma((1,)),
        ],
        compiler_params=pltpu.CompilerParams(
            collective_id=0, has_side_effects=True, vmem_limit_bytes=60 * 1024 * 1024
        ),
    )(p_start, r_start, diag_shift, shifts, block_values, block_cols.T, live_slots, needed)
    return pl.pallas_call(
        deliver,
        out_shape=results,
        in_specs=[vmem, vmem],
        out_specs=(hbm, hbm),
        scratch_shapes=[dma((2,))],
        compiler_params=pltpu.CompilerParams(vmem_limit_bytes=4 * 1024 * 1024),
    )(basis, gram)


def solution(mesh):
    both = ("group", "dom")
    in_specs = (
        P(both, None),
        P(both, None),
        P(both, None),
        P(),
        P(both, None, None, None),
        P(both, None),
        P(both),
        P(both, None, None),
    )
    return jax.shard_map(
        functools.partial(per_device, mesh.shape["group"], mesh.shape["dom"]),
        mesh=mesh,
        in_specs=in_specs,
        out_specs=(P(None, both, None), P()),
        check_vma=False,
    )
```

```python
import functools

import jax
import jax.numpy as jnp
from jax import lax
from jax.experimental import pallas as pl
from jax.experimental.pallas import tpu as pltpu
from jax.sharding import PartitionSpec as P

MESH = pl.DeviceIdType.MESH
UNROLL = 32
TOGETHER = 4
EARLY = 8
GROWS = 24
COLUMN = 8


def split(x):
    high = x.astype(jnp.bfloat16)
    low = (x - high.astype(jnp.float32)).astype(jnp.bfloat16)
    return high, low


def both_halves(x):
    high, low = split(x)
    return jnp.concatenate([high, low], axis=0)


def four_sum(y, bs):
    return (y[8:16, bs:] + y[8:16, :bs]) + (y[0:8, bs:] + y[0:8, :bs])


def kernel(
    rows, slots, bs, halo, depth, n_group, n_dom,
    p_hbm, r_hbm, diag_hbm, shifts_hbm, values_hbm, cols_hbm, live_hbm, needed_hbm,
    out, gram_out,
    shifts, cols, live, needed, wanted, stage, weights, ext_a, ext_b, fields, start, diag, index, partial, own, parcel, lists, lists_in,
    gram_mine, gram_in_a, gram_in_b, row_mine, row_in,
    value_sem, small_sem, send_sem, recv_sem, gram_send, gram_recv, row_send, row_recv, list_send, list_recv,
):
    g = lax.axis_index("group")
    m = lax.axis_index("dom")
    n_x = n_dom // COLUMN
    x, w = m // COLUMN, m % COLUMN
    width = 2 * rows
    nothing = 5 * width

    small = [
        pltpu.make_async_copy(p_hbm, start.at[0], small_sem.at[0]),
        pltpu.make_async_copy(r_hbm, start.at[1], small_sem.at[1]),
        pltpu.make_async_copy(diag_hbm, diag, small_sem.at[2]),
        pltpu.make_async_copy(cols_hbm, cols, small_sem.at[3]),
        pltpu.make_async_copy(live_hbm, live, small_sem.at[4]),
        pltpu.make_async_copy(needed_hbm, needed, small_sem.at[5]),
        pltpu.make_async_copy(shifts_hbm, shifts, small_sem.at[6]),
        pltpu.make_async_copy(needed_hbm, lists, small_sem.at[7]),
    ]
    neighbours = (
        (g, (m + n_dom - 1) % n_dom),
        (g, (m + 1) % n_dom),
        ((g + n_group - 1) % n_group, m),
        ((g + 1) % n_group, m),
    )
    peers_a = [(g, x * COLUMN + (w + j) % COLUMN) for j in range(1, COLUMN)]
    peers_b = [
        ((g + j // n_x) % n_group, (x + j) % n_x * COLUMN + w) for j in range(1, n_x * n_group)
    ]
    def hops(offset, size):
        return min(offset, size - offset)

    sorted_b = [
        peers_b[j - 1]
        for j in sorted(
            range(1, n_x * n_group), key=lambda j: -(hops(j // n_x, n_group) + hops(j % n_x, n_x))
        )
    ]

    before, after = m > 0, m < n_dom - 1

    def where_there(k, act):
        if k < 2:
            pl.when((before, after)[k])(act)
        else:
            act()

    lists_in[...] = jnp.zeros(lists_in.shape, jnp.int32)
    barrier = pltpu.get_barrier_semaphore()

    def greet(peer):
        pl.semaphore_signal(barrier, inc=1, device_id=peer, device_id_type=MESH)

    for peer in sorted_b + peers_a:
        greet(peer)
    for k in range(2):
        where_there(k, functools.partial(greet, neighbours[k]))
    for copy in small:
        copy.start()
    greetings = len(peers_a + peers_b) + before.astype(jnp.int32) + after.astype(jnp.int32)

    def value_copy(b):
        return pltpu.make_async_copy(values_hbm.at[b], stage.at[b], value_sem.at[b])

    def start_values(b, carry):
        value_copy(b).start()
        return carry

    lax.fori_loop(0, rows, start_values, 0)

    for copy in small:
        copy.wait()
    for ext in (ext_a, ext_b):
        ext[nothing : nothing + 16, :] = jnp.zeros((16, bs), jnp.float32)
    ext_a[pl.ds(0, rows, stride=2), :] = start[0]
    ext_a[pl.ds(1, rows, stride=2), :] = start[1]
    fields[...] = jnp.zeros(fields.shape, jnp.float32)

    def whole_copy(k, landing):
        return pltpu.make_async_remote_copy(
            src_ref=ext_a.at[0:width],
            dst_ref=ext_a.at[(1 + landing) * width : (2 + landing) * width],
            send_sem=send_sem.at[8 + k],
            recv_sem=recv_sem.at[8 + landing],
            device_id=neighbours[k],
            device_id_type=MESH,
        )

    def list_copy(k, landing):
        return pltpu.make_async_remote_copy(
            src_ref=lists,
            dst_ref=lists_in.at[landing : landing + 1],
            send_sem=list_send.at[k],
            recv_sem=list_recv.at[landing],
            device_id=neighbours[k],
            device_id_type=MESH,
        )

    def field_copy(ext, parity, k, landing):
        span = 2 * halo
        return pltpu.make_async_remote_copy(
            src_ref=parcel.at[k],
            dst_ref=ext.at[width + landing * span : width + (1 + landing) * span],
            send_sem=send_sem.at[4 * parity + k],
            recv_sem=recv_sem.at[4 * parity + landing],
            device_id=neighbours[k],
            device_id_type=MESH,
        )

    def send_all(copy_of):
        for k in (2, 3, 0, 1):
            where_there(k, copy_of(k, k ^ 1).start)

    def await_all(copy_of):
        for k in range(4):
            where_there(k, copy_of(k, k).wait_recv)
        for k in range(4):
            where_there(k, copy_of(k, k ^ 1).wait_send)

    def send_field(ext, parity):
        for k in range(4):
            for h in range(halo):
                block = wanted[k, k ^ 1, h]
                parcel[k, 2 * h : 2 * h + 2, :] = own[pl.ds(2 * block, 2), :]
        send_all(functools.partial(field_copy, ext, parity))

    def await_field(ext, parity):
        await_all(functools.partial(field_copy, ext, parity))

    def prepare_one(b):
        for s in range(slots):
            high, low = split(stage[b, s].T)
            weights[b, 0, s * bs : (s + 1) * bs, :] = high
            weights[b, 1, s * bs : (s + 1) * bs, :] = low
        used = live[b]
        for s in range(1, slots):
            c = cols[s, b]
            far = jnp.maximum(c - rows, 0)
            k, h = far // halo, far % halo
            spot = jnp.where(c < rows, c, (1 + k) * rows + needed[0, k, h])
            index[b * slots + s] = jnp.where(s < used, 2 * spot, nothing)
            index[(rows + b) * slots + s] = jnp.where(s < used, 2 * c, nothing)

    def prepare(i, carry):
        for u in range(TOGETHER):
            value_copy(i * TOGETHER + u).wait()
        for u in range(TOGETHER):
            prepare_one(i * TOGETHER + u)
        return carry

    lax.fori_loop(0, EARLY // TOGETHER, prepare, 0)
    pl.semaphore_wait(barrier, greetings)
    send_all(whole_copy)
    send_all(list_copy)
    lax.fori_loop(EARLY // TOGETHER, rows // TOGETHER, prepare, 0)

    def matrix(b, first, last):
        span = slice(first * bs, last * bs)
        return jnp.concatenate([weights[b, 0, span, :], weights[b, 1, span, :]], axis=1)

    def keep(src, step):
        out[step] = src[pl.ds(0, rows, stride=2), :]
        r_row = jnp.where(step < depth, depth + 1 + step, GROWS - 1)

        @pl.when(step < depth)
        def _():
            out[depth + 1 + step] = src[pl.ds(1, rows, stride=2), :]

        for b in range(rows):
            fields[b, pl.ds(step, 1), :] = src[2 * b : 2 * b + 1, :]
            fields[b, pl.ds(r_row, 1), :] = src[2 * b + 1 : 2 * b + 2, :]

    def ahead(src, step):
        theta = shifts[step]
        for first in range(0, rows, 4):
            own = src[2 * first : 2 * first + 8, :]
            lhs = both_halves(own)
            for j in range(4):
                b, two = first + j, slice(2 * j, 2 * j + 2)
                y = jnp.dot(lhs, matrix(b, 0, 1), preferred_element_type=jnp.float32)
                near = four_sum(y, bs)[two] + (diag[b : b + 1, :] - theta) * own[two]
                partial[2 * b : 2 * b + 2, :] = near

    def advance(src, dst, table):
        def some(i, carry):
            for u in range(UNROLL):
                b = i * UNROLL + u
                lhs = jnp.concatenate(
                    [
                        both_halves(src[pl.ds(index[(table * rows + b) * slots + s], 8), :])
                        for s in range(1, slots)
                    ],
                    axis=1,
                )
                y = jnp.dot(lhs, matrix(b, 1, slots), preferred_element_type=jnp.float32)
                new = four_sum(y, bs)[0:2] + partial[pl.ds(2 * b, 2), :]
                dst[pl.ds(2 * b, 2), :] = new
                own[pl.ds(2 * b, 2), :] = new
            return carry

        lax.fori_loop(0, rows // UNROLL, some, 0)

    def gram_part():
        highs, lows = [], []
        for b in range(rows):
            high, low = split(fields[b])
            highs.append(high)
            lows.append(low)
        both = jnp.concatenate(
            [jnp.concatenate(highs, axis=1), jnp.concatenate(lows, axis=1)], axis=0
        )
        prod = lax.dot_general(
            both, both, (((1,), (1,)), ((), ())), preferred_element_type=jnp.float32
        )
        gram = (prod[GROWS:, GROWS:] + prod[GROWS:, :GROWS]) + (
            prod[:GROWS, GROWS:] + prod[:GROWS, :GROWS]
        )
        gram_mine[0] = jnp.zeros((8, bs), jnp.float32)
        for i in range(GROWS // 8):
            gram_mine[0, :, 32 * i : 32 * i + GROWS] = gram[8 * i : 8 * i + 8]

    rounds = (
        (peers_a, w, gram_in_a, 0),
        (peers_b, g * n_x + x, gram_in_b, COLUMN),
    )

    def round_copies(number):
        peers, mine, landing, first = rounds[number]
        return [
            pltpu.make_async_remote_copy(
                src_ref=gram_mine.at[number],
                dst_ref=landing.at[mine],
                send_sem=gram_send.at[first + j],
                recv_sem=gram_recv.at[first + j],
                device_id=peer,
                device_id_type=MESH,
            )
            for j, peer in enumerate(peers)
        ]

    def start_round(number):
        _, mine, landing, _ = rounds[number]
        for copy in round_copies(number):
            copy.start()
        landing[mine] = gram_mine[number]

    def end_round(number):
        peers, _, landing, _ = rounds[number]
        for copy in round_copies(number):
            copy.wait()
        total = landing[0]
        for i in range(1, len(peers) + 1):
            total = total + landing[i]
        return total

    ahead(ext_a, 0)
    keep(ext_a, 0)
    await_all(list_copy)
    fetch = pltpu.make_async_copy(lists_in, wanted, small_sem.at[0])
    fetch.start()
    fetch.wait()

    def pair(i, carry):
        @pl.when(i == 0)
        def _():
            await_all(whole_copy)

        @pl.when(i > 0)
        def _():
            await_field(ext_a, 0)

        advance(ext_a, ext_b, jnp.minimum(i, 1))
        send_field(ext_b, 1)
        ahead(ext_b, 2 * i + 1)
        keep(ext_b, 2 * i + 1)

        @pl.when(i == depth // 2 - 1)
        def _():
            gram_part()
            start_round(0)

        await_field(ext_b, 1)
        advance(ext_b, ext_a, 1)

        @pl.when(i < depth // 2 - 1)
        def _():
            send_field(ext_a, 0)
            ahead(ext_a, 2 * i + 2)

        keep(ext_a, 2 * i + 2)
        return carry

    lax.fori_loop(0, depth // 2, pair, 0)

    last = jnp.zeros((GROWS, bs), jnp.float32)
    for b in range(rows):
        last = last + fields[b] * ext_a[2 * b : 2 * b + 1, :]
    row_mine[...] = jnp.zeros((1, bs), jnp.float32)
    row_mine[:, 0:GROWS] = jnp.sum(last.T, axis=0, keepdims=True)
    count = n_group * n_dom
    me = g * n_dom + m

    offsets = sorted(
        ((dg, dx) for dg in range(n_group) for dx in range(n_x)),
        key=lambda o: -(hops(o[0], n_group) + hops(o[1], n_x)),
    )
    for dg, dx in offsets:

        def send_row(j, carry, to_g=(g + dg) % n_group, to_x=(x + dx) % n_x):
            pltpu.make_async_remote_copy(
                src_ref=row_mine,
                dst_ref=row_in.at[me],
                send_sem=row_send.at[0],
                recv_sem=row_recv.at[0],
                device_id=(to_g, to_x * COLUMN + (w + j) % COLUMN),
                device_id_type=MESH,
            ).start()
            return carry

        for j in range(0 if dg or dx else 1, COLUMN):
            send_row(j, 0)
    row_in[me] = row_mine[...]

    gram_mine[1] = end_round(0)
    start_round(1)
    total = end_round(1)

    rows_sent = pltpu.make_async_remote_copy(
        src_ref=row_in.at[0 : count - 1],
        dst_ref=row_in.at[0 : count - 1],
        send_sem=row_send.at[0],
        recv_sem=row_recv.at[0],
        device_id=neighbours[3],
        device_id_type=MESH,
    )
    rows_sent.wait_recv()
    rows_sent.wait_send()
    sums = [row_in[i] for i in range(8)]
    for i in range(8, count):
        sums[i % 8] = sums[i % 8] + row_in[i]
    while len(sums) > 1:
        sums = [a + b for a, b in zip(sums[0::2], sums[1::2])]
    row = sums[0]

    scale = 1.0 / (rows * bs * count)
    ncols = 2 * depth + 1
    across = jnp.broadcast_to(row, (bs, bs))
    down = across.T
    for i in range(0, ncols, 8):
        some = min(8, ncols - i)
        part = total[0:some, 4 * i : 4 * i + ncols]
        r = i + lax.broadcasted_iota(jnp.int32, (some, ncols), 0)
        c = lax.broadcasted_iota(jnp.int32, (some, ncols), 1)
        part = jnp.where(c == depth, down[i : i + some, 0:ncols], part)
        part = jnp.where(r == depth, across[i : i + some, 0:ncols], part)
        gram_out[i : i + some, :] = part * scale


def deliver(basis, gram, basis_out, gram_out, sems):
    copies = [
        pltpu.make_async_copy(basis, basis_out, sems.at[0]),
        pltpu.make_async_copy(gram, gram_out, sems.at[1]),
    ]
    for copy in copies:
        copy.start()
    for copy in copies:
        copy.wait()


def per_device(n_group, n_dom, p_start, r_start, diag_shift, shifts, block_values, block_cols, live_slots, needed):
    rows, bs = p_start.shape
    slots = block_cols.shape[1]
    halo = needed.shape[2]
    depth = shifts.shape[0]
    ncols = 2 * depth + 1
    f32 = jnp.float32
    hbm = pl.BlockSpec(memory_space=pltpu.HBM)
    dma = pltpu.SemaphoreType.DMA
    peers_b = n_group * n_dom // COLUMN
    vmem = pl.BlockSpec(memory_space=pltpu.VMEM)
    results = (
        jax.ShapeDtypeStruct((ncols, rows, bs), f32),
        jax.ShapeDtypeStruct((ncols, ncols), f32),
    )
    basis, gram = pl.pallas_call(
        functools.partial(kernel, rows, slots, bs, halo, depth, n_group, n_dom),
        out_shape=tuple(pltpu.VMEM(r.shape, r.dtype) for r in results),
        in_specs=[hbm] * 8,
        out_specs=(vmem, vmem),
        scratch_shapes=[
            pltpu.SMEM((depth,), f32),
            pltpu.SMEM((slots, rows), jnp.int32),
            pltpu.SMEM((rows,), jnp.int32),
            pltpu.SMEM((1, 4, halo), jnp.int32),
            pltpu.SMEM((4, 4, halo), jnp.int32),
            pltpu.VMEM((rows, slots, bs, bs), f32),
            pltpu.VMEM((rows, 2, slots * bs, bs), jnp.bfloat16),
            pltpu.VMEM((10 * rows + 16, bs), f32),
            pltpu.VMEM((10 * rows + 16, bs), f32),
            pltpu.VMEM((rows, GROWS, bs), f32),
            pltpu.VMEM((2, rows, bs), f32),
            pltpu.VMEM((rows, bs), f32),
            pltpu.SMEM((2 * rows * slots,), jnp.int32),
            pltpu.VMEM((2 * rows, bs), f32),
            pltpu.VMEM((2 * rows, bs), f32),
            pltpu.VMEM((4, 2 * halo, bs), f32),
            pltpu.VMEM((1, 4, halo), jnp.int32),
            pltpu.VMEM((4, 4, halo), jnp.int32),
            pltpu.VMEM((2, 8, bs), f32),
            pltpu.VMEM((COLUMN, 8, bs), f32),
            pltpu.VMEM((peers_b, 8, bs), f32),
            pltpu.VMEM((1, bs), f32),
            pltpu.VMEM((n_group * n_dom, 1, bs), f32),
            dma((rows,)),
            dma((8,)),
            dma((12,)),
            dma((12,)),
            dma((COLUMN + peers_b,)),
            dma((COLUMN + peers_b,)),
            dma((1,)),
            dma((1,)),
            dma((4,)),
            dma((4,)),
        ],
        compiler_params=pltpu.CompilerParams(
            collective_id=0, has_side_effects=True, vmem_limit_bytes=60 * 1024 * 1024
        ),
    )(p_start, r_start, diag_shift, shifts, block_values, block_cols.T, live_slots, needed)
    return pl.pallas_call(
        deliver,
        out_shape=results,
        in_specs=[vmem, vmem],
        out_specs=(hbm, hbm),
        scratch_shapes=[dma((2,))],
        compiler_params=pltpu.CompilerParams(vmem_limit_bytes=4 * 1024 * 1024),
    )(basis, gram)


def solution(mesh):
    both = ("group", "dom")
    in_specs = (
        P(both, None),
        P(both, None),
        P(both, None),
        P(),
        P(both, None, None, None),
        P(both, None),
        P(both),
        P(both, None, None),
    )
    return jax.shard_map(
        functools.partial(per_device, mesh.shape["group"], mesh.shape["dom"]),
        mesh=mesh,
        in_specs=in_specs,
        out_specs=(P(None, both, None), P()),
        check_vma=False,
    )
```

```python
import functools

import jax
import jax.numpy as jnp
from jax import lax
from jax.experimental import pallas as pl
from jax.experimental.pallas import tpu as pltpu
from jax.sharding import PartitionSpec as P

MESH = pl.DeviceIdType.MESH
UNROLL = 32
TOGETHER = 4
EARLY = 8
GROWS = 24
COLUMN = 8


def split(x):
    high = x.astype(jnp.bfloat16)
    low = (x - high.astype(jnp.float32)).astype(jnp.bfloat16)
    return high, low


def both_halves(x):
    high, low = split(x)
    return jnp.concatenate([high, low], axis=0)


def four_sum(y, bs):
    return (y[8:16, bs:] + y[8:16, :bs]) + (y[0:8, bs:] + y[0:8, :bs])


def kernel(
    rows, slots, bs, halo, depth, n_group, n_dom,
    p_hbm, r_hbm, diag_hbm, shifts_hbm, values_hbm, cols_hbm, live_hbm, needed_hbm,
    out, gram_out,
    shifts, cols, live, needed, wanted, stage, weights, ext_a, ext_b, fields, start, diag, index, partial, own, parcel, lists, lists_in,
    gram_mine, gram_in_a, gram_in_b, row_mine, row_in,
    value_sem, small_sem, send_sem, recv_sem, gram_send, gram_recv, row_send, row_recv, list_send, list_recv,
):
    g = lax.axis_index("group")
    m = lax.axis_index("dom")
    n_x = n_dom // COLUMN
    x, w = m // COLUMN, m % COLUMN
    width = 2 * rows
    nothing = 5 * width

    small = [
        pltpu.make_async_copy(p_hbm, start.at[0], small_sem.at[0]),
        pltpu.make_async_copy(r_hbm, start.at[1], small_sem.at[1]),
        pltpu.make_async_copy(diag_hbm, diag, small_sem.at[2]),
        pltpu.make_async_copy(cols_hbm, cols, small_sem.at[3]),
        pltpu.make_async_copy(live_hbm, live, small_sem.at[4]),
        pltpu.make_async_copy(needed_hbm, needed, small_sem.at[5]),
        pltpu.make_async_copy(shifts_hbm, shifts, small_sem.at[6]),
        pltpu.make_async_copy(needed_hbm, lists, small_sem.at[7]),
    ]
    neighbours = (
        (g, (m + n_dom - 1) % n_dom),
        (g, (m + 1) % n_dom),
        ((g + n_group - 1) % n_group, m),
        ((g + 1) % n_group, m),
    )
    peers_a = [(g, x * COLUMN + (w + j) % COLUMN) for j in range(1, COLUMN)]
    peers_b = [
        ((g + j // n_x) % n_group, (x + j) % n_x * COLUMN + w) for j in range(1, n_x * n_group)
    ]
    def hops(offset, size):
        return min(offset, size - offset)

    sorted_b = [
        peers_b[j - 1]
        for j in sorted(
            range(1, n_x * n_group), key=lambda j: -(hops(j // n_x, n_group) + hops(j % n_x, n_x))
        )
    ]

    before, after = m > 0, m < n_dom - 1

    def where_there(k, act):
        if k < 2:
            pl.when((before, after)[k])(act)
        else:
            act()

    lists_in[...] = jnp.zeros(lists_in.shape, jnp.int32)
    barrier = pltpu.get_barrier_semaphore()

    def greet(peer):
        pl.semaphore_signal(barrier, inc=1, device_id=peer, device_id_type=MESH)

    for peer in sorted_b + peers_a:
        greet(peer)
    for k in range(2):
        where_there(k, functools.partial(greet, neighbours[k]))
    for copy in small:
        copy.start()
    greetings = len(peers_a + peers_b) + before.astype(jnp.int32) + after.astype(jnp.int32)

    def value_copy(b):
        return pltpu.make_async_copy(values_hbm.at[b], stage.at[b], value_sem.at[b])

    def start_values(b, carry):
        value_copy(b).start()
        return carry

    lax.fori_loop(0, rows, start_values, 0)

    for copy in small:
        copy.wait()
    for ext in (ext_a, ext_b):
        ext[nothing : nothing + 16, :] = jnp.zeros((16, bs), jnp.float32)
    ext_a[pl.ds(0, rows, stride=2), :] = start[0]
    ext_a[pl.ds(1, rows, stride=2), :] = start[1]
    fields[...] = jnp.zeros(fields.shape, jnp.float32)

    def whole_copy(k, landing):
        return pltpu.make_async_remote_copy(
            src_ref=ext_a.at[0:width],
            dst_ref=ext_a.at[(1 + landing) * width : (2 + landing) * width],
            send_sem=send_sem.at[8 + k],
            recv_sem=recv_sem.at[8 + landing],
            device_id=neighbours[k],
            device_id_type=MESH,
        )

    def list_copy(k, landing):
        return pltpu.make_async_remote_copy(
            src_ref=lists,
            dst_ref=lists_in.at[landing : landing + 1],
            send_sem=list_send.at[k],
            recv_sem=list_recv.at[landing],
            device_id=neighbours[k],
            device_id_type=MESH,
        )

    def field_copy(ext, parity, k, landing):
        span = 2 * halo
        return pltpu.make_async_remote_copy(
            src_ref=parcel.at[k],
            dst_ref=ext.at[width + landing * span : width + (1 + landing) * span],
            send_sem=send_sem.at[4 * parity + k],
            recv_sem=recv_sem.at[4 * parity + landing],
            device_id=neighbours[k],
            device_id_type=MESH,
        )

    def send_all(copy_of):
        for k in (2, 3, 0, 1):
            where_there(k, copy_of(k, k ^ 1).start)

    def await_all(copy_of):
        for k in range(4):
            where_there(k, copy_of(k, k).wait_recv)
        for k in range(4):
            where_there(k, copy_of(k, k ^ 1).wait_send)

    def send_field(ext, parity):
        for k in range(4):
            for h in range(halo):
                block = wanted[k, k ^ 1, h]
                parcel[k, 2 * h : 2 * h + 2, :] = own[pl.ds(2 * block, 2), :]
        send_all(functools.partial(field_copy, ext, parity))

    def await_field(ext, parity):
        await_all(functools.partial(field_copy, ext, parity))

    def prepare_one(b):
        for s in range(slots):
            high, low = split(stage[b, s].T)
            weights[b, 0, s * bs : (s + 1) * bs, :] = high
            weights[b, 1, s * bs : (s + 1) * bs, :] = low
        used = live[b]
        for s in range(1, slots):
            c = cols[s, b]
            far = jnp.maximum(c - rows, 0)
            k, h = far // halo, far % halo
            spot = jnp.where(c < rows, c, (1 + k) * rows + needed[0, k, h])
            index[b * slots + s] = jnp.where(s < used, 2 * spot, nothing)
            index[(rows + b) * slots + s] = jnp.where(s < used, 2 * c, nothing)

    def prepare(i, carry):
        for u in range(TOGETHER):
            value_copy(i * TOGETHER + u).wait()
        for u in range(TOGETHER):
            prepare_one(i * TOGETHER + u)
        return carry

    lax.fori_loop(0, EARLY // TOGETHER, prepare, 0)
    pl.semaphore_wait(barrier, greetings)
    send_all(whole_copy)
    send_all(list_copy)
    lax.fori_loop(EARLY // TOGETHER, rows // TOGETHER, prepare, 0)

    def matrix(b, first, last):
        span = slice(first * bs, last * bs)
        return jnp.concatenate([weights[b, 0, span, :], weights[b, 1, span, :]], axis=1)

    def keep(src, step):
        out[step] = src[pl.ds(0, rows, stride=2), :]
        r_row = jnp.where(step < depth, depth + 1 + step, GROWS - 1)

        @pl.when(step < depth)
        def _():
            out[depth + 1 + step] = src[pl.ds(1, rows, stride=2), :]

        for b in range(rows):
            fields[b, pl.ds(step, 1), :] = src[2 * b : 2 * b + 1, :]
            fields[b, pl.ds(r_row, 1), :] = src[2 * b + 1 : 2 * b + 2, :]

    def ahead(src, step):
        theta = shifts[step]
        for first in range(0, rows, 4):
            own = src[2 * first : 2 * first + 8, :]
            lhs = both_halves(own)
            for j in range(4):
                b, two = first + j, slice(2 * j, 2 * j + 2)
                y = jnp.dot(lhs, matrix(b, 0, 1), preferred_element_type=jnp.float32)
                near = four_sum(y, bs)[two] + (diag[b : b + 1, :] - theta) * own[two]
                partial[2 * b : 2 * b + 2, :] = near

    def advance(src, dst, table):
        def some(i, carry):
            for u in range(UNROLL):
                b = i * UNROLL + u
                lhs = jnp.concatenate(
                    [
                        both_halves(src[pl.ds(index[(table * rows + b) * slots + s], 8), :])
                        for s in range(1, slots)
                    ],
                    axis=1,
                )
                y = jnp.dot(lhs, matrix(b, 1, slots), preferred_element_type=jnp.float32)
                new = four_sum(y, bs)[0:2] + partial[pl.ds(2 * b, 2), :]
                dst[pl.ds(2 * b, 2), :] = new
                own[pl.ds(2 * b, 2), :] = new
            return carry

        lax.fori_loop(0, rows // UNROLL, some, 0)

    def gram_part():
        highs, lows = [], []
        for b in range(rows):
            high, low = split(fields[b])
            highs.append(high)
            lows.append(low)
        both = jnp.concatenate(
            [jnp.concatenate(highs, axis=1), jnp.concatenate(lows, axis=1)], axis=0
        )
        prod = lax.dot_general(
            both, both, (((1,), (1,)), ((), ())), preferred_element_type=jnp.float32
        )
        gram = (prod[GROWS:, GROWS:] + prod[GROWS:, :GROWS]) + (
            prod[:GROWS, GROWS:] + prod[:GROWS, :GROWS]
        )
        gram_mine[0] = jnp.zeros((8, bs), jnp.float32)
        for i in range(GROWS // 8):
            gram_mine[0, :, 32 * i : 32 * i + GROWS] = gram[8 * i : 8 * i + 8]

    rounds = (
        (peers_a, w, gram_in_a, 0),
        (peers_b, g * n_x + x, gram_in_b, COLUMN),
    )

    def round_copies(number):
        peers, mine, landing, first = rounds[number]
        return [
            pltpu.make_async_remote_copy(
                src_ref=gram_mine.at[number],
                dst_ref=landing.at[mine],
                send_sem=gram_send.at[first + j],
                recv_sem=gram_recv.at[first + j],
                device_id=peer,
                device_id_type=MESH,
            )
            for j, peer in enumerate(peers)
        ]

    def start_round(number):
        _, mine, landing, _ = rounds[number]
        for copy in round_copies(number):
            copy.start()
        landing[mine] = gram_mine[number]

    def end_round(number):
        peers, _, landing, _ = rounds[number]
        for copy in round_copies(number):
            copy.wait()
        total = landing[0]
        for i in range(1, len(peers) + 1):
            total = total + landing[i]
        return total

    ahead(ext_a, 0)
    keep(ext_a, 0)
    await_all(list_copy)
    fetch = pltpu.make_async_copy(lists_in, wanted, small_sem.at[0])
    fetch.start()
    fetch.wait()

    def pair(i, carry):
        @pl.when(i == 0)
        def _():
            await_all(whole_copy)

        @pl.when(i > 0)
        def _():
            await_field(ext_a, 0)

        advance(ext_a, ext_b, jnp.minimum(i, 1))
        send_field(ext_b, 1)
        ahead(ext_b, 2 * i + 1)
        keep(ext_b, 2 * i + 1)

        @pl.when(i == depth // 2 - 1)
        def _():
            gram_part()
            start_round(0)

        await_field(ext_b, 1)
        advance(ext_b, ext_a, 1)

        @pl.when(i < depth // 2 - 1)
        def _():
            send_field(ext_a, 0)
            ahead(ext_a, 2 * i + 2)

            keep(ext_a, 2 * i + 2)

        return carry

    lax.fori_loop(0, depth // 2, pair, 0)

    last = jnp.zeros((GROWS, bs), jnp.float32)
    square = jnp.zeros((1, bs), jnp.float32)
    for b in range(rows):
        new = ext_a[2 * b : 2 * b + 1, :]
        last = last + fields[b] * new
        square = square + new * new
    at = lax.broadcasted_iota(jnp.int32, (GROWS, bs), 0)
    last = jnp.where(at == depth, square, last)
    row_mine[...] = jnp.zeros((1, bs), jnp.float32)
    row_mine[:, 0:GROWS] = jnp.sum(last.T, axis=0, keepdims=True)
    count = n_group * n_dom
    me = g * n_dom + m

    offsets = sorted(
        ((dg, dx) for dg in range(n_group) for dx in range(n_x)),
        key=lambda o: -(hops(o[0], n_group) + hops(o[1], n_x)),
    )
    for dg, dx in offsets:

        def send_row(j, carry, to_g=(g + dg) % n_group, to_x=(x + dx) % n_x):
            pltpu.make_async_remote_copy(
                src_ref=row_mine,
                dst_ref=row_in.at[me],
                send_sem=row_send.at[0],
                recv_sem=row_recv.at[0],
                device_id=(to_g, to_x * COLUMN + (w + j) % COLUMN),
                device_id_type=MESH,
            ).start()
            return carry

        for j in range(0 if dg or dx else 1, COLUMN):
            send_row(j, 0)
    row_in[me] = row_mine[...]
    out[depth] = ext_a[pl.ds(0, rows, stride=2), :]

    gram_mine[1] = end_round(0)
    start_round(1)
    total = end_round(1)

    rows_sent = pltpu.make_async_remote_copy(
        src_ref=row_in.at[0 : count - 1],
        dst_ref=row_in.at[0 : count - 1],
        send_sem=row_send.at[0],
        recv_sem=row_recv.at[0],
        device_id=neighbours[3],
        device_id_type=MESH,
    )
    rows_sent.wait_recv()
    rows_sent.wait_send()
    sums = [row_in[i] for i in range(8)]
    for i in range(8, count):
        sums[i % 8] = sums[i % 8] + row_in[i]
    while len(sums) > 1:
        sums = [a + b for a, b in zip(sums[0::2], sums[1::2])]
    row = sums[0]

    scale = 1.0 / (rows * bs * count)
    ncols = 2 * depth + 1
    across = jnp.broadcast_to(row, (bs, bs))
    down = across.T
    for i in range(0, ncols, 8):
        some = min(8, ncols - i)
        part = total[0:some, 4 * i : 4 * i + ncols]
        r = i + lax.broadcasted_iota(jnp.int32, (some, ncols), 0)
        c = lax.broadcasted_iota(jnp.int32, (some, ncols), 1)
        part = jnp.where(c == depth, down[i : i + some, 0:ncols], part)
        part = jnp.where(r == depth, across[i : i + some, 0:ncols], part)
        gram_out[i : i + some, :] = part * scale


def deliver(basis, gram, basis_out, gram_out, sems):
    copies = [
        pltpu.make_async_copy(basis, basis_out, sems.at[0]),
        pltpu.make_async_copy(gram, gram_out, sems.at[1]),
    ]
    for copy in copies:
        copy.start()
    for copy in copies:
        copy.wait()


def per_device(n_group, n_dom, p_start, r_start, diag_shift, shifts, block_values, block_cols, live_slots, needed):
    rows, bs = p_start.shape
    slots = block_cols.shape[1]
    halo = needed.shape[2]
    depth = shifts.shape[0]
    ncols = 2 * depth + 1
    f32 = jnp.float32
    hbm = pl.BlockSpec(memory_space=pltpu.HBM)
    dma = pltpu.SemaphoreType.DMA
    peers_b = n_group * n_dom // COLUMN
    vmem = pl.BlockSpec(memory_space=pltpu.VMEM)
    results = (
        jax.ShapeDtypeStruct((ncols, rows, bs), f32),
        jax.ShapeDtypeStruct((ncols, ncols), f32),
    )
    basis, gram = pl.pallas_call(
        functools.partial(kernel, rows, slots, bs, halo, depth, n_group, n_dom),
        out_shape=tuple(pltpu.VMEM(r.shape, r.dtype) for r in results),
        in_specs=[hbm] * 8,
        out_specs=(vmem, vmem),
        scratch_shapes=[
            pltpu.SMEM((depth,), f32),
            pltpu.SMEM((slots, rows), jnp.int32),
            pltpu.SMEM((rows,), jnp.int32),
            pltpu.SMEM((1, 4, halo), jnp.int32),
            pltpu.SMEM((4, 4, halo), jnp.int32),
            pltpu.VMEM((rows, slots, bs, bs), f32),
            pltpu.VMEM((rows, 2, slots * bs, bs), jnp.bfloat16),
            pltpu.VMEM((10 * rows + 16, bs), f32),
            pltpu.VMEM((10 * rows + 16, bs), f32),
            pltpu.VMEM((rows, GROWS, bs), f32),
            pltpu.VMEM((2, rows, bs), f32),
            pltpu.VMEM((rows, bs), f32),
            pltpu.SMEM((2 * rows * slots,), jnp.int32),
            pltpu.VMEM((2 * rows, bs), f32),
            pltpu.VMEM((2 * rows, bs), f32),
            pltpu.VMEM((4, 2 * halo, bs), f32),
            pltpu.VMEM((1, 4, halo), jnp.int32),
            pltpu.VMEM((4, 4, halo), jnp.int32),
            pltpu.VMEM((2, 8, bs), f32),
            pltpu.VMEM((COLUMN, 8, bs), f32),
            pltpu.VMEM((peers_b, 8, bs), f32),
            pltpu.VMEM((1, bs), f32),
            pltpu.VMEM((n_group * n_dom, 1, bs), f32),
            dma((rows,)),
            dma((8,)),
            dma((12,)),
            dma((12,)),
            dma((COLUMN + peers_b,)),
            dma((COLUMN + peers_b,)),
            dma((1,)),
            dma((1,)),
            dma((4,)),
            dma((4,)),
        ],
        compiler_params=pltpu.CompilerParams(
            collective_id=0, has_side_effects=True, vmem_limit_bytes=60 * 1024 * 1024
        ),
    )(p_start, r_start, diag_shift, shifts, block_values, block_cols.T, live_slots, needed)
    return pl.pallas_call(
        deliver,
        out_shape=results,
        in_specs=[vmem, vmem],
        out_specs=(hbm, hbm),
        scratch_shapes=[dma((2,))],
        compiler_params=pltpu.CompilerParams(vmem_limit_bytes=4 * 1024 * 1024),
    )(basis, gram)


def solution(mesh):
    both = ("group", "dom")
    in_specs = (
        P(both, None),
        P(both, None),
        P(both, None),
        P(),
        P(both, None, None, None),
        P(both, None),
        P(both),
        P(both, None, None),
    )
    return jax.shard_map(
        functools.partial(per_device, mesh.shape["group"], mesh.shape["dom"]),
        mesh=mesh,
        in_specs=in_specs,
        out_specs=(P(None, both, None), P()),
        check_vma=False,
    )
```

```python
import functools

import jax
import jax.numpy as jnp
from jax import lax
from jax.experimental import pallas as pl
from jax.experimental.pallas import tpu as pltpu
from jax.sharding import PartitionSpec as P

MESH = pl.DeviceIdType.MESH
UNROLL = 32
TOGETHER = 4
EARLY = 8
GROWS = 24
COLUMN = 8


def split(x):
    high = x.astype(jnp.bfloat16)
    low = (x - high.astype(jnp.float32)).astype(jnp.bfloat16)
    return high, low


def both_halves(x):
    high, low = split(x)
    return jnp.concatenate([high, low], axis=0)


def four_sum(y, bs):
    return (y[8:16, bs:] + y[8:16, :bs]) + (y[0:8, bs:] + y[0:8, :bs])


def kernel(
    rows, slots, bs, halo, depth, n_group, n_dom,
    p_hbm, r_hbm, diag_hbm, shifts_hbm, values_hbm, cols_hbm, live_hbm, needed_hbm,
    out, gram_out,
    shifts, cols, live, needed, wanted, stage, weights, ext_a, ext_b, fields, start, diag, index, partial, own, parcel, lists, lists_in,
    gram_mine, gram_in_a, gram_in_b, row_mine, row_in,
    value_sem, small_sem, send_sem, recv_sem, gram_send, gram_recv, row_send, row_recv, list_send, list_recv,
):
    g = lax.axis_index("group")
    m = lax.axis_index("dom")
    n_x = n_dom // COLUMN
    x, w = m // COLUMN, m % COLUMN
    width = 2 * rows
    nothing = 5 * width

    small = [
        pltpu.make_async_copy(p_hbm, start.at[0], small_sem.at[0]),
        pltpu.make_async_copy(r_hbm, start.at[1], small_sem.at[1]),
        pltpu.make_async_copy(diag_hbm, diag, small_sem.at[2]),
        pltpu.make_async_copy(cols_hbm, cols, small_sem.at[3]),
        pltpu.make_async_copy(live_hbm, live, small_sem.at[4]),
        pltpu.make_async_copy(needed_hbm, needed, small_sem.at[5]),
        pltpu.make_async_copy(shifts_hbm, shifts, small_sem.at[6]),
        pltpu.make_async_copy(needed_hbm, lists, small_sem.at[7]),
    ]
    neighbours = (
        (g, (m + n_dom - 1) % n_dom),
        (g, (m + 1) % n_dom),
        ((g + n_group - 1) % n_group, m),
        ((g + 1) % n_group, m),
    )
    peers_a = [(g, x * COLUMN + (w + j) % COLUMN) for j in range(1, COLUMN)]
    peers_b = [
        ((g + j // n_x) % n_group, (x + j) % n_x * COLUMN + w) for j in range(1, n_x * n_group)
    ]
    def hops(offset, size):
        return min(offset, size - offset)

    sorted_b = [
        peers_b[j - 1]
        for j in sorted(
            range(1, n_x * n_group), key=lambda j: -(hops(j // n_x, n_group) + hops(j % n_x, n_x))
        )
    ]

    before, after = m > 0, m < n_dom - 1

    def where_there(k, act):
        if k < 2:
            pl.when((before, after)[k])(act)
        else:
            act()

    lists_in[...] = jnp.zeros(lists_in.shape, jnp.int32)
    barrier = pltpu.get_barrier_semaphore()

    def greet(peer):
        pl.semaphore_signal(barrier, inc=1, device_id=peer, device_id_type=MESH)

    for peer in sorted_b + peers_a:
        greet(peer)
    for k in range(2):
        where_there(k, functools.partial(greet, neighbours[k]))
    for copy in small:
        copy.start()
    greetings = len(peers_a + peers_b) + before.astype(jnp.int32) + after.astype(jnp.int32)

    def value_copy(b):
        return pltpu.make_async_copy(values_hbm.at[b], stage.at[b], value_sem.at[b])

    def start_values(b, carry):
        value_copy(b).start()
        return carry

    lax.fori_loop(0, rows, start_values, 0)

    for copy in small:
        copy.wait()
    for ext in (ext_a, ext_b):
        ext[nothing : nothing + 16, :] = jnp.zeros((16, bs), jnp.float32)
    ext_a[pl.ds(0, rows, stride=2), :] = start[0]
    ext_a[pl.ds(1, rows, stride=2), :] = start[1]
    fields[...] = jnp.zeros(fields.shape, jnp.float32)

    def whole_copy(k, landing):
        return pltpu.make_async_remote_copy(
            src_ref=ext_a.at[0:width],
            dst_ref=ext_a.at[(1 + landing) * width : (2 + landing) * width],
            send_sem=send_sem.at[8 + k],
            recv_sem=recv_sem.at[8 + landing],
            device_id=neighbours[k],
            device_id_type=MESH,
        )

    def list_copy(k, landing):
        return pltpu.make_async_remote_copy(
            src_ref=lists,
            dst_ref=lists_in.at[landing : landing + 1],
            send_sem=list_send.at[k],
            recv_sem=list_recv.at[landing],
            device_id=neighbours[k],
            device_id_type=MESH,
        )

    def field_copy(ext, parity, k, landing):
        span = 2 * halo
        return pltpu.make_async_remote_copy(
            src_ref=parcel.at[k],
            dst_ref=ext.at[width + landing * span : width + (1 + landing) * span],
            send_sem=send_sem.at[4 * parity + k],
            recv_sem=recv_sem.at[4 * parity + landing],
            device_id=neighbours[k],
            device_id_type=MESH,
        )

    def send_all(copy_of):
        for k in (2, 3, 0, 1):
            where_there(k, copy_of(k, k ^ 1).start)

    def await_all(copy_of):
        for k in range(4):
            where_there(k, copy_of(k, k).wait_recv)
        for k in range(4):
            where_there(k, copy_of(k, k ^ 1).wait_send)

    def send_field(ext, parity):
        for k in range(4):
            for h in range(halo):
                block = wanted[k, k ^ 1, h]
                parcel[k, 2 * h : 2 * h + 2, :] = own[pl.ds(2 * block, 2), :]
        send_all(functools.partial(field_copy, ext, parity))

    def await_field(ext, parity):
        await_all(functools.partial(field_copy, ext, parity))

    def prepare_one(b):
        for s in range(slots):
            high, low = split(stage[b, s].T)
            weights[b, 0, s * bs : (s + 1) * bs, :] = high
            weights[b, 1, s * bs : (s + 1) * bs, :] = low
        used = live[b]
        for s in range(1, slots):
            c = cols[s, b]
            far = jnp.maximum(c - rows, 0)
            k, h = far // halo, far % halo
            spot = jnp.where(c < rows, c, (1 + k) * rows + needed[0, k, h])
            index[b * slots + s] = jnp.where(s < used, 2 * spot, nothing)
            index[(rows + b) * slots + s] = jnp.where(s < used, 2 * c, nothing)

    def prepare(i, carry):
        for u in range(TOGETHER):
            value_copy(i * TOGETHER + u).wait()
        for u in range(TOGETHER):
            prepare_one(i * TOGETHER + u)
        return carry

    lax.fori_loop(0, EARLY // TOGETHER, prepare, 0)
    pl.semaphore_wait(barrier, greetings)
    send_all(whole_copy)
    send_all(list_copy)
    lax.fori_loop(EARLY // TOGETHER, rows // TOGETHER, prepare, 0)

    def matrix(b, first, last):
        span = slice(first * bs, last * bs)
        return jnp.concatenate([weights[b, 0, span, :], weights[b, 1, span, :]], axis=1)

    def keep(src, step):
        out[step] = src[pl.ds(0, rows, stride=2), :]
        r_row = jnp.where(step < depth, depth + 1 + step, GROWS - 1)

        @pl.when(step < depth)
        def _():
            out[depth + 1 + step] = src[pl.ds(1, rows, stride=2), :]

        for b in range(rows):
            fields[b, pl.ds(step, 1), :] = src[2 * b : 2 * b + 1, :]
            fields[b, pl.ds(r_row, 1), :] = src[2 * b + 1 : 2 * b + 2, :]

    def ahead(src, step):
        theta = shifts[step]
        for first in range(0, rows, 4):
            own = src[2 * first : 2 * first + 8, :]
            lhs = both_halves(own)
            for j in range(4):
                b, two = first + j, slice(2 * j, 2 * j + 2)
                y = jnp.dot(lhs, matrix(b, 0, 1), preferred_element_type=jnp.float32)
                near = four_sum(y, bs)[two] + (diag[b : b + 1, :] - theta) * own[two]
                partial[2 * b : 2 * b + 2, :] = near

    def advance(src, dst, table):
        def some(i, carry):
            for u in range(UNROLL):
                b = i * UNROLL + u
                lhs = jnp.concatenate(
                    [
                        both_halves(src[pl.ds(index[(table * rows + b) * slots + s], 8), :])
                        for s in range(1, slots)
                    ],
                    axis=1,
                )
                y = jnp.dot(lhs, matrix(b, 1, slots), preferred_element_type=jnp.float32)
                new = four_sum(y, bs)[0:2] + partial[pl.ds(2 * b, 2), :]
                dst[pl.ds(2 * b, 2), :] = new
                own[pl.ds(2 * b, 2), :] = new
            return carry

        lax.fori_loop(0, rows // UNROLL, some, 0)

    def gram_part():
        highs, lows = [], []
        for b in range(rows):
            high, low = split(fields[b])
            highs.append(high)
            lows.append(low)
        both = jnp.concatenate(
            [jnp.concatenate(highs, axis=1), jnp.concatenate(lows, axis=1)], axis=0
        )
        prod = lax.dot_general(
            both, both, (((1,), (1,)), ((), ())), preferred_element_type=jnp.float32
        )
        gram = (prod[GROWS:, GROWS:] + prod[GROWS:, :GROWS]) + (
            prod[:GROWS, GROWS:] + prod[:GROWS, :GROWS]
        )
        gram_mine[0] = jnp.zeros((8, bs), jnp.float32)
        for i in range(GROWS // 8):
            gram_mine[0, :, 32 * i : 32 * i + GROWS] = gram[8 * i : 8 * i + 8]

    rounds = (
        (peers_a, w, gram_in_a, 0),
        (peers_b, g * n_x + x, gram_in_b, COLUMN),
    )

    def round_copies(number):
        peers, mine, landing, first = rounds[number]
        return [
            pltpu.make_async_remote_copy(
                src_ref=gram_mine.at[number],
                dst_ref=landing.at[mine],
                send_sem=gram_send.at[first + j],
                recv_sem=gram_recv.at[first + j],
                device_id=peer,
                device_id_type=MESH,
            )
            for j, peer in enumerate(peers)
        ]

    def start_round(number):
        _, mine, landing, _ = rounds[number]
        for copy in round_copies(number):
            copy.start()
        landing[mine] = gram_mine[number]

    def end_round(number):
        peers, _, landing, _ = rounds[number]
        for copy in round_copies(number):
            copy.wait()
        total = landing[0]
        for i in range(1, len(peers) + 1):
            total = total + landing[i]
        return total

    ahead(ext_a, 0)
    keep(ext_a, 0)
    await_all(list_copy)
    fetch = pltpu.make_async_copy(lists_in, wanted, small_sem.at[0])
    fetch.start()
    fetch.wait()

    def pair(i, carry):
        @pl.when(i == 0)
        def _():
            await_all(whole_copy)

        @pl.when(i > 0)
        def _():
            await_field(ext_a, 0)

        advance(ext_a, ext_b, jnp.minimum(i, 1))
        send_field(ext_b, 1)
        ahead(ext_b, 2 * i + 1)
        keep(ext_b, 2 * i + 1)

        @pl.when(i == depth // 2 - 1)
        def _():
            gram_part()
            start_round(0)

        await_field(ext_b, 1)
        advance(ext_b, ext_a, 1)

        @pl.when(i < depth // 2 - 1)
        def _():
            send_field(ext_a, 0)
            ahead(ext_a, 2 * i + 2)

            keep(ext_a, 2 * i + 2)

        return carry

    lax.fori_loop(0, depth // 2, pair, 0)

    lasts = [jnp.zeros((GROWS, bs), jnp.float32)] * 4
    square = jnp.zeros((1, bs), jnp.float32)
    for b in range(rows):
        new = ext_a[2 * b : 2 * b + 1, :]
        lasts[b % 4] = lasts[b % 4] + fields[b] * new
        square = square + new * new
    last = (lasts[0] + lasts[1]) + (lasts[2] + lasts[3])
    at = lax.broadcasted_iota(jnp.int32, (GROWS, bs), 0)
    last = jnp.where(at == depth, square, last)
    row_mine[...] = jnp.zeros((1, bs), jnp.float32)
    row_mine[:, 0:GROWS] = jnp.sum(last.T, axis=0, keepdims=True)
    count = n_group * n_dom
    me = g * n_dom + m

    offsets = sorted(
        ((dg, dx) for dg in range(n_group) for dx in range(n_x)),
        key=lambda o: -(hops(o[0], n_group) + hops(o[1], n_x)),
    )
    for dg, dx in offsets:

        def send_row(j, carry, to_g=(g + dg) % n_group, to_x=(x + dx) % n_x):
            pltpu.make_async_remote_copy(
                src_ref=row_mine,
                dst_ref=row_in.at[me],
                send_sem=row_send.at[0],
                recv_sem=row_recv.at[0],
                device_id=(to_g, to_x * COLUMN + (w + j) % COLUMN),
                device_id_type=MESH,
            ).start()
            return carry

        for j in range(0 if dg or dx else 1, COLUMN):
            send_row(j, 0)
    row_in[me] = row_mine[...]
    out[depth] = ext_a[pl.ds(0, rows, stride=2), :]

    gram_mine[1] = end_round(0)
    start_round(1)
    total = end_round(1)

    rows_sent = pltpu.make_async_remote_copy(
        src_ref=row_in.at[0 : count - 1],
        dst_ref=row_in.at[0 : count - 1],
        send_sem=row_send.at[0],
        recv_sem=row_recv.at[0],
        device_id=neighbours[3],
        device_id_type=MESH,
    )
    rows_sent.wait_recv()
    rows_sent.wait_send()
    sums = [row_in[i] for i in range(8)]
    for i in range(8, count):
        sums[i % 8] = sums[i % 8] + row_in[i]
    while len(sums) > 1:
        sums = [a + b for a, b in zip(sums[0::2], sums[1::2])]
    row = sums[0]

    scale = 1.0 / (rows * bs * count)
    ncols = 2 * depth + 1
    across = jnp.broadcast_to(row, (bs, bs))
    down = across.T
    for i in range(0, ncols, 8):
        some = min(8, ncols - i)
        part = total[0:some, 4 * i : 4 * i + ncols]
        r = i + lax.broadcasted_iota(jnp.int32, (some, ncols), 0)
        c = lax.broadcasted_iota(jnp.int32, (some, ncols), 1)
        part = jnp.where(c == depth, down[i : i + some, 0:ncols], part)
        part = jnp.where(r == depth, across[i : i + some, 0:ncols], part)
        gram_out[i : i + some, :] = part * scale


def deliver(basis, gram, basis_out, gram_out, sems):
    copies = [
        pltpu.make_async_copy(basis, basis_out, sems.at[0]),
        pltpu.make_async_copy(gram, gram_out, sems.at[1]),
    ]
    for copy in copies:
        copy.start()
    for copy in copies:
        copy.wait()


def per_device(n_group, n_dom, p_start, r_start, diag_shift, shifts, block_values, block_cols, live_slots, needed):
    rows, bs = p_start.shape
    slots = block_cols.shape[1]
    halo = needed.shape[2]
    depth = shifts.shape[0]
    ncols = 2 * depth + 1
    f32 = jnp.float32
    hbm = pl.BlockSpec(memory_space=pltpu.HBM)
    dma = pltpu.SemaphoreType.DMA
    peers_b = n_group * n_dom // COLUMN
    vmem = pl.BlockSpec(memory_space=pltpu.VMEM)
    results = (
        jax.ShapeDtypeStruct((ncols, rows, bs), f32),
        jax.ShapeDtypeStruct((ncols, ncols), f32),
    )
    basis, gram = pl.pallas_call(
        functools.partial(kernel, rows, slots, bs, halo, depth, n_group, n_dom),
        out_shape=tuple(pltpu.VMEM(r.shape, r.dtype) for r in results),
        in_specs=[hbm] * 8,
        out_specs=(vmem, vmem),
        scratch_shapes=[
            pltpu.SMEM((depth,), f32),
            pltpu.SMEM((slots, rows), jnp.int32),
            pltpu.SMEM((rows,), jnp.int32),
            pltpu.SMEM((1, 4, halo), jnp.int32),
            pltpu.SMEM((4, 4, halo), jnp.int32),
            pltpu.VMEM((rows, slots, bs, bs), f32),
            pltpu.VMEM((rows, 2, slots * bs, bs), jnp.bfloat16),
            pltpu.VMEM((10 * rows + 16, bs), f32),
            pltpu.VMEM((10 * rows + 16, bs), f32),
            pltpu.VMEM((rows, GROWS, bs), f32),
            pltpu.VMEM((2, rows, bs), f32),
            pltpu.VMEM((rows, bs), f32),
            pltpu.SMEM((2 * rows * slots,), jnp.int32),
            pltpu.VMEM((2 * rows, bs), f32),
            pltpu.VMEM((2 * rows, bs), f32),
            pltpu.VMEM((4, 2 * halo, bs), f32),
            pltpu.VMEM((1, 4, halo), jnp.int32),
            pltpu.VMEM((4, 4, halo), jnp.int32),
            pltpu.VMEM((2, 8, bs), f32),
            pltpu.VMEM((COLUMN, 8, bs), f32),
            pltpu.VMEM((peers_b, 8, bs), f32),
            pltpu.VMEM((1, bs), f32),
            pltpu.VMEM((n_group * n_dom, 1, bs), f32),
            dma((rows,)),
            dma((8,)),
            dma((12,)),
            dma((12,)),
            dma((COLUMN + peers_b,)),
            dma((COLUMN + peers_b,)),
            dma((1,)),
            dma((1,)),
            dma((4,)),
            dma((4,)),
        ],
        compiler_params=pltpu.CompilerParams(
            collective_id=0, has_side_effects=True, vmem_limit_bytes=60 * 1024 * 1024
        ),
    )(p_start, r_start, diag_shift, shifts, block_values, block_cols.T, live_slots, needed)
    return pl.pallas_call(
        deliver,
        out_shape=results,
        in_specs=[vmem, vmem],
        out_specs=(hbm, hbm),
        scratch_shapes=[dma((2,))],
        compiler_params=pltpu.CompilerParams(vmem_limit_bytes=4 * 1024 * 1024),
    )(basis, gram)


def solution(mesh):
    both = ("group", "dom")
    in_specs = (
        P(both, None),
        P(both, None),
        P(both, None),
        P(),
        P(both, None, None, None),
        P(both, None),
        P(both),
        P(both, None, None),
    )
    return jax.shard_map(
        functools.partial(per_device, mesh.shape["group"], mesh.shape["dom"]),
        mesh=mesh,
        in_specs=in_specs,
        out_specs=(P(None, both, None), P()),
        check_vma=False,
    )
```
